32 devices in a mesh: dp: 2 (over x), tx: 4 (over z), ty: 4 (over y, core).
Axes of the slice: x: 2, y: 2, z: 4, core: 2. Of those that a mesh axis runs over, the one named last changes fastest.
Arguments:
- x_in: bfloat16 [64, 256, 1152], P('dp', None, 'tx'), parts along dimension 0
- ln1_gain: float32 [2, 1152], P(None, 'tx')
- ln1_bias: float32 [2, 1152], P(None, 'tx')
- w_q: bfloat16 [2, 1152, 16, 72], P(None, 'tx', 'ty')
- b_q: float32 [2, 16, 72], P(None, 'ty')
- w_k: bfloat16 [2, 1152, 16, 72], P(None, 'tx', 'ty')
- w_v: bfloat16 [2, 1152, 16, 72], P(None, 'tx', 'ty')
- b_v: float32 [2, 16, 72], P(None, 'ty')
- w_o: bfloat16 [2, 16, 72, 1152], P(None, 'ty', None, 'tx')
- b_o: float32 [2, 1152], P(None, 'tx')
- ln2_gain: float32 [2, 1152], P(None, 'tx')
- ln2_bias: float32 [2, 1152], P(None, 'tx')
- w_up: bfloat16 [2, 1152, 4304], P(None, 'tx', 'ty')
- b_up: float32 [2, 4304], P(None, 'ty')
- w_down: bfloat16 [2, 4304, 1152], P(None, 'ty', 'tx')
- b_down: float32 [2, 1152], P(None, 'tx')
Outputs:
- output: bfloat16 [64, 256, 1152], P('dp', None, 'tx'), parts along dimension 0
There are 2 independent parts. The reference program is written for one: setup_inputs(seed, part) draws one part's arguments, and reference() takes and returns one part's arrays. A program takes and returns all parts, laid end to end along the dimension named above; an argument that names none is the same for every part.
All inputs are finite; a program needn't handle non-finite values.
Results may differ from the reference program's by a relative error of at most 0.02.
Values are sent between devices in bfloat16 or wider.
A program may use at most 1 GiB of HBM per device.

```python
import jax
import jax.numpy as jnp
from jax import lax

IMGS = 32
N = 256
W = 1152
HEADS = 16
HEAD = 72
F = 4304
EPS = 1e-6


def setup_inputs(seed: int = 0, part: int = 0) -> dict:
    key = jax.random.key(seed)
    keys = jax.random.split(key, 16)
    act_keys = jax.random.split(jax.random.fold_in(key, part), 3)
    col_mean = 0.5 * jax.random.normal(act_keys[0], (W,), jnp.float32)
    col_scale = jnp.exp(0.5 * jax.random.normal(act_keys[1], (W,), jnp.float32))
    x_vals = jax.random.normal(act_keys[2], (IMGS, N, W), jnp.float32) * col_scale + col_mean
    w_scale = W ** -0.5
    f_scale = F ** -0.5

    def draw(index, shape, scale):
        return scale * jax.random.normal(keys[index], shape, jnp.float32)

    return {
        "x_in": x_vals.astype(jnp.bfloat16),
        "ln1_gain": 1.0 + draw(0, (2, W), 0.3),
        "ln1_bias": draw(1, (2, W), 0.3),
        "w_q": draw(2, (2, W, HEADS, HEAD), 1.7 * w_scale).astype(jnp.bfloat16),
        "b_q": draw(3, (2, HEADS, HEAD), 0.5),
        "w_k": draw(4, (2, W, HEADS, HEAD), 1.7 * w_scale).astype(jnp.bfloat16),
        "w_v": draw(5, (2, W, HEADS, HEAD), w_scale).astype(jnp.bfloat16),
        "b_v": draw(6, (2, HEADS, HEAD), 0.5),
        "w_o": draw(7, (2, HEADS, HEAD, W), w_scale).astype(jnp.bfloat16),
        "b_o": draw(8, (2, W), 0.3),
        "ln2_gain": 1.0 + draw(9, (2, W), 0.3),
        "ln2_bias": draw(10, (2, W), 0.3),
        "w_up": draw(11, (2, W, F), w_scale).astype(jnp.bfloat16),
        "b_up": draw(12, (2, F), 0.5),
        "w_down": draw(13, (2, F, W), f_scale).astype(jnp.bfloat16),
        "b_down": draw(14, (2, W), 0.3),
    }


def layer_norm(x_f, gain, shift):
    mean = jnp.mean(x_f, axis=-1, keepdims=True)
    centred = x_f - mean
    variance = jnp.mean(centred * centred, axis=-1, keepdims=True)
    return (centred * lax.rsqrt(variance + EPS) * gain + shift).astype(jnp.bfloat16)


def encoder_layer(x_img, params):
    (ln1_gain, ln1_bias, w_q, b_q, w_k, w_v, b_v, w_o, b_o,
     ln2_gain, ln2_bias, w_up, b_up, w_down, b_down) = params
    x_f = x_img.astype(jnp.float32)
    normed = layer_norm(x_f, ln1_gain, ln1_bias)
    q_proj = (jnp.dot(normed, w_q.reshape(W, W), preferred_element_type=jnp.float32) + b_q.reshape(W)).astype(jnp.bfloat16)
    k_proj = jnp.dot(normed, w_k.reshape(W, W), preferred_element_type=jnp.float32).astype(jnp.bfloat16)
    v_proj = (jnp.dot(normed, w_v.reshape(W, W), preferred_element_type=jnp.float32) + b_v.reshape(W)).astype(jnp.bfloat16)
    q_heads = q_proj.reshape(N, HEADS, HEAD).astype(jnp.float32)
    k_heads = k_proj.reshape(N, HEADS, HEAD).astype(jnp.float32)
    v_heads = v_proj.reshape(N, HEADS, HEAD).astype(jnp.float32)
    scores = jnp.einsum("qhd,khd->hqk", q_heads, k_heads) * (HEAD ** -0.5)
    attn_prob = jax.nn.softmax(scores, axis=-1).astype(jnp.bfloat16)
    attended = jnp.einsum("hqk,khd->qhd", attn_prob.astype(jnp.float32), v_heads).astype(jnp.bfloat16)
    x_mid = (x_f + jnp.dot(attended.reshape(N, W), w_o.reshape(W, W), preferred_element_type=jnp.float32) + b_o).astype(jnp.bfloat16)
    mid_f = x_mid.astype(jnp.float32)
    normed2 = layer_norm(mid_f, ln2_gain, ln2_bias)
    hidden = jax.nn.gelu(jnp.dot(normed2, w_up, preferred_element_type=jnp.float32) + b_up, approximate=True).astype(jnp.bfloat16)
    x_out = (mid_f + jnp.dot(hidden, w_down, preferred_element_type=jnp.float32) + b_down).astype(jnp.bfloat16)
    return x_out, None


def reference(x_in, ln1_gain, ln1_bias, w_q, b_q, w_k, w_v, b_v, w_o, b_o, ln2_gain, ln2_bias, w_up, b_up, w_down, b_down):
    params = (ln1_gain, ln1_bias, w_q, b_q, w_k, w_v, b_v, w_o, b_o,
              ln2_gain, ln2_bias, w_up, b_up, w_down, b_down)

    def run_image(x_img):
        x_last, _ = lax.scan(encoder_layer, x_img, params)
        return x_last

    return lax.map(run_image, x_in)
```

```python
import jax
import jax.numpy as jnp
from jax import lax
from jax.experimental import pallas as pl
from jax.experimental.pallas import tpu as pltpu
from jax.sharding import PartitionSpec as P

EPS = 1e-6
BF = jnp.bfloat16
F32 = jnp.float32
LANES = 128
VMEM_BYTES = 60 * 1024 * 1024


def norm_rows(x_f, gain, shift):
    mean = jnp.mean(x_f, axis=-1, keepdims=True)
    centred = x_f - mean
    variance = jnp.mean(centred * centred, axis=-1, keepdims=True)
    return (centred * lax.rsqrt(variance + EPS) * gain + shift).astype(BF)


def dot_nn(a, b):
    return lax.dot_general(a, b, (((1,), (0,)), ((), ())), preferred_element_type=F32)


def dot_nt(a, b):
    return lax.dot_general(a, b, (((1,), (1,)), ((), ())), preferred_element_type=F32)


def attention_kernel(heads, dim, toks, x_ref, gain_ref, shift_ref, bias_ref, bo_ref, w_ref, out_ref, h_ref, acc_ref):
    step = pl.program_id(0)
    width = x_ref.shape[-1]
    hd = heads * dim
    span = -(-hd // LANES) * LANES

    @pl.when(step == 0)
    def _():
        h_ref[...] = norm_rows(x_ref[...].astype(F32), gain_ref[...], shift_ref[...])
        acc_ref[...] = jnp.zeros_like(acc_ref)

    w = w_ref[...].reshape(width, w_ref.shape[-1])
    cols = w.shape[-1]
    qkv = dot_nn(h_ref[...], w) + bias_ref[0]
    q_f = qkv[:, :span]
    k = pltpu.roll(qkv, cols - hd, 1)[:, :span].astype(BF)
    v = pltpu.roll(qkv, hd, 1)[:, cols - span:].astype(BF)
    lane = lax.broadcasted_iota(jnp.int32, (toks, span), 1)
    outs = []
    for img in range(x_ref.shape[0] // toks):
        rows = slice(img * toks, (img + 1) * toks)
        q_i, k_i, v_i = q_f[rows], k[rows], v[rows]
        o_i = jnp.zeros((toks, span), F32)
        for head in range(heads):
            q_h = jnp.where((lane >= head * dim) & (lane < (head + 1) * dim), q_i, 0.0).astype(BF)
            s = dot_nt(q_h, k_i) * (dim ** -0.5)
            e = jnp.exp(s - jnp.max(s, axis=-1, keepdims=True))
            p = (e / jnp.sum(e, axis=-1, keepdims=True)).astype(BF)
            lo = span - hd + head * dim
            o_i = jnp.where((lane >= lo) & (lane < lo + dim), dot_nn(p, v_i), o_i)
        outs.append(o_i)
    acc_ref[...] += dot_nt(jnp.concatenate(outs, axis=0).astype(BF), w[:, cols - span:])

    @pl.when(step == pl.num_programs(0) - 1)
    def _():
        out_ref[...] = (x_ref[...].astype(F32) + acc_ref[...] + bo_ref[...]).astype(BF)


def mlp_kernel(toks, x_ref, gain_ref, shift_ref, bias_ref, bd_ref, up_ref, down_ref, out_ref, h_ref, acc_ref):
    step = pl.program_id(0)
    width = x_ref.shape[-1]

    @pl.when(step == 0)
    def _():
        h_ref[...] = norm_rows(x_ref[...].astype(F32), gain_ref[...], shift_ref[...])
        acc_ref[...] = jnp.zeros_like(acc_ref)

    up = up_ref[...].reshape(width, up_ref.shape[-1])
    down = down_ref[...].reshape(width, down_ref.shape[-1])
    u = jax.nn.gelu(dot_nn(h_ref[...], up) + bias_ref[0], approximate=True).astype(BF)
    acc_ref[...] += dot_nt(u, down)

    @pl.when(step == pl.num_programs(0) - 1)
    def _():
        y = x_ref[...].astype(F32) + acc_ref[...] + bd_ref[...]
        if out_ref.shape == x_ref.shape:
            out_ref[...] = y.astype(BF)
        else:
            wl = out_ref.shape[2]
            y_t = y.T.astype(BF)
            for c in range(out_ref.shape[0]):
                for img in range(out_ref.shape[1]):
                    out_ref[c, img] = y_t[c * wl:(c + 1) * wl, img * toks:(img + 1) * toks]


def solution(mesh):
    tx, ty = mesh.shape["tx"], mesh.shape["ty"]
    act_spec = P("dp", None, "tx")
    vec_tx = P(None, "tx")
    proj_spec = P(None, "tx", "ty", None)
    head_vec = P(None, "ty", None)
    in_specs = (act_spec, vec_tx, vec_tx, proj_spec, head_vec, proj_spec, proj_spec, head_vec,
                P(None, "ty", None, "tx"), vec_tx, vec_tx, vec_tx,
                P(None, "tx", "ty"), P(None, "ty"), P(None, "ty", "tx"), vec_tx)

    def local_fn(x_in, ln1_gain, ln1_bias, w_q, b_q, w_k, w_v, b_v, w_o, b_o, ln2_gain, ln2_bias, w_up, b_up, w_down, b_down):
        layers, wl, hl, dim = w_q.shape
        fl = w_up.shape[-1]
        imgs, toks, _ = x_in.shape
        hd = hl * dim
        width = wl * tx
        cols = max(4 * hd, -(-fl // LANES) * LANES)
        per = imgs // ty
        nb = per // tx
        n = nb * toks

        def proj_block(l):
            rows = [w[l].transpose(1, 2, 0).reshape(hd, wl) for w in (w_q, w_k, w_v)] + [w_o[l].reshape(hd, wl)]
            return jnp.pad(jnp.concatenate(rows, axis=0).T, ((0, 0), (0, cols - 4 * hd)))

        def up_block(l):
            return jnp.pad(w_up[l], ((0, 0), (0, cols - fl)))

        def down_block(l):
            return jnp.pad(w_down[l].T, ((0, 0), (0, cols - fl)))

        blocks = []
        for l in range(layers):
            blocks += [("a", l, proj_block), ("u", l, up_block), ("d", l, down_block)]
        where = {}
        gathered = []
        for i in range(0, len(blocks), 2):
            pair = blocks[i:i + 2]
            for j, (kind, l, _) in enumerate(pair):
                where[kind, l] = (len(gathered), j)
            with jax.named_scope(f"gather{i // 2}"):
                local = jnp.stack([make(l) for _, l, make in pair])
                full = lax.all_gather(local.reshape(len(pair) * wl, cols), ("tx", "ty"), axis=0)
            gathered.append(full.reshape(tx, ty, len(pair), wl, cols))

        with jax.named_scope("entry"):
            mine = lax.dynamic_slice_in_dim(x_in.transpose(0, 2, 1), lax.axis_index("ty") * per, per, axis=0)
            x_t = lax.all_to_all(mine, "tx", split_axis=0, concat_axis=0, tiled=True)
            x = x_t.reshape(tx, nb, wl, toks).transpose(1, 3, 0, 2).reshape(n, width)
        with jax.named_scope("vectors"):
            on_tx = [ln1_gain, ln1_bias, ln2_gain, ln2_bias, b_o, b_down]
            on_ty = [b_q.reshape(layers, hd), b_v.reshape(layers, hd), b_up]
            vec = lax.all_gather(jnp.concatenate([a.reshape(1, -1) for a in on_tx + on_ty], axis=1), ("tx", "ty"), axis=0)
            vec = vec.reshape(tx, ty, -1)
            at = len(on_tx) * layers * wl
            vt = vec[:, 0, :at].reshape(tx, len(on_tx), layers, wl).transpose(1, 2, 0, 3).reshape(len(on_tx), layers, 1, width)
            vq = vec[0, :, at:at + layers * hd].reshape(ty, layers, hd)
            vv = vec[0, :, at + layers * hd:at + 2 * layers * hd].reshape(ty, layers, hd)
            vu = vec[0, :, at + 2 * layers * hd:].reshape(ty, layers, fl)
            gap = jnp.zeros_like(vq)
            tail = jnp.zeros((ty, layers, cols - 4 * hd), F32)
            bias_a = jnp.concatenate([vq, gap, vv, gap, tail], axis=2).transpose(1, 0, 2).reshape(layers, ty, 1, cols)
            bias_u = jnp.pad(vu, ((0, 0), (0, 0), (0, cols - fl))).transpose(1, 0, 2).reshape(layers, ty, 1, cols)

        whole = pl.BlockSpec((n, width), lambda i: (0, 0))
        row = pl.BlockSpec((1, width), lambda i: (0, 0))
        bias = pl.BlockSpec((1, 1, cols), lambda i: (i, 0, 0))
        scratch = [pltpu.VMEM((n, width), BF), pltpu.VMEM((n, width), F32)]
        params = pltpu.CompilerParams(vmem_limit_bytes=VMEM_BYTES, dimension_semantics=("arbitrary",))

        def weight(kind, l):
            g, j = where[kind, l]
            return gathered[g], pl.BlockSpec((tx, 1, 1, wl, cols), lambda i: (0, i, j, 0, 0))

        for l in range(layers):
            w_a, spec_a = weight("a", l)
            with jax.named_scope(f"attention{l}"):
                x = pl.pallas_call(
                    lambda *refs: attention_kernel(hl, dim, toks, *refs),
                    grid=(ty,),
                    in_specs=[whole, row, row, bias, row, spec_a],
                    out_specs=whole,
                    out_shape=jax.ShapeDtypeStruct((n, width), BF),
                    scratch_shapes=scratch,
                    compiler_params=params,
                    name="attention",
                    cost_estimate=pl.CostEstimate(flops=2 * n * width * width * 5, bytes_accessed=2 * width * width * 4, transcendentals=n * toks * 16),
                )(x, vt[0, l], vt[1, l], bias_a[l], vt[4, l], w_a)
            w_u, spec_u = weight("u", l)
            w_d, spec_d = weight("d", l)
            last = l == layers - 1
            out = (tx, nb, wl, toks) if last else (n, width)
            with jax.named_scope(f"mlp{l}"):
                x = pl.pallas_call(
                    lambda *refs: mlp_kernel(toks, *refs),
                    grid=(ty,),
                    in_specs=[whole, row, row, bias, row, spec_u, spec_d],
                    out_specs=pl.BlockSpec(out, lambda i, r=len(out): (0,) * r),
                    out_shape=jax.ShapeDtypeStruct(out, BF),
                    scratch_shapes=scratch,
                    compiler_params=params,
                    name="mlp",
                    cost_estimate=pl.CostEstimate(flops=2 * n * width * cols * ty * 2, bytes_accessed=4 * width * cols * ty, transcendentals=n * cols * ty),
                )(x, vt[2, l], vt[3, l], bias_u[l], vt[5, l], w_u, w_d)
        with jax.named_scope("exit"):
            y = lax.all_to_all(x.reshape(tx * nb, wl, toks), "tx", split_axis=0, concat_axis=0, tiled=True)
            y = lax.all_gather(y, "ty", axis=0, tiled=True)
        return y.transpose(0, 2, 1)

    return jax.shard_map(local_fn, mesh=mesh, in_specs=in_specs, out_specs=act_spec, check_vma=False)
```

```python
import jax
import jax.numpy as jnp
from jax import lax
from jax.experimental import pallas as pl
from jax.experimental.pallas import tpu as pltpu
from jax.sharding import PartitionSpec as P


EPS = 1e-6
BF = jnp.bfloat16
F32 = jnp.float32
LANES = 128
VMEM_BYTES = 60 * 1024 * 1024
RING_ROWS = 456


def norm_rows(x_f, gain, shift):
    mean = jnp.mean(x_f, axis=-1, keepdims=True)
    centred = x_f - mean
    variance = jnp.mean(centred * centred, axis=-1, keepdims=True)
    return (centred * lax.rsqrt(variance + EPS) * gain + shift).astype(BF)


def dot_nn(a, b):
    return lax.dot_general(a, b, (((1,), (0,)), ((), ())), preferred_element_type=F32)


def dot_nt(a, b):
    return lax.dot_general(a, b, (((1,), (1,)), ((), ())), preferred_element_type=F32)


def attention_kernel(heads, dim, toks, x_ref, gain_ref, shift_ref, bias_ref, bo_ref, w_ref, out_ref, h_ref, acc_ref):
    step = pl.program_id(0)
    width = x_ref.shape[-1]
    hd = heads * dim
    span = -(-hd // LANES) * LANES

    @pl.when(step == 0)
    def _():
        h_ref[...] = norm_rows(x_ref[...].astype(F32), gain_ref[...], shift_ref[...])
        acc_ref[...] = jnp.zeros_like(acc_ref)

    w = w_ref[...].reshape(width, w_ref.shape[-1])
    cols = w.shape[-1]
    qkv = dot_nn(h_ref[...], w) + bias_ref[0]
    q_f = qkv[:, :span]
    k = pltpu.roll(qkv, cols - hd, 1)[:, :span].astype(BF)
    v = pltpu.roll(qkv, hd, 1)[:, cols - span:].astype(BF)
    lane = lax.broadcasted_iota(jnp.int32, (toks, span), 1)
    outs = []
    for img in range(x_ref.shape[0] // toks):
        rows = slice(img * toks, (img + 1) * toks)
        q_i, k_i, v_i = q_f[rows], k[rows], v[rows]
        o_i = jnp.zeros((toks, span), F32)
        for head in range(heads):
            q_h = jnp.where((lane >= head * dim) & (lane < (head + 1) * dim), q_i, 0.0).astype(BF)
            s = dot_nt(q_h, k_i) * (dim ** -0.5)
            e = jnp.exp(s - jnp.max(s, axis=-1, keepdims=True))
            p = (e / jnp.sum(e, axis=-1, keepdims=True)).astype(BF)
            lo = span - hd + head * dim
            o_i = jnp.where((lane >= lo) & (lane < lo + dim), dot_nn(p, v_i), o_i)
        outs.append(o_i)
    acc_ref[...] += dot_nt(jnp.concatenate(outs, axis=0).astype(BF), w[:, cols - span:])

    @pl.when(step == pl.num_programs(0) - 1)
    def _():
        out_ref[...] = (x_ref[...].astype(F32) + acc_ref[...] + bo_ref[...]).astype(BF)


def mlp_kernel(toks, up_kind, down_kind, x_ref, gain_ref, shift_ref, bias_ref, bd_ref, *rest):
    counts = [1 if kind is None else 3 for kind in (up_kind, down_kind)]
    srcs = (rest[:counts[0]], rest[counts[0]:sum(counts)])
    out_ref, h_ref, acc_ref, up_buf, down_buf, sems = rest[sum(counts):]
    step = pl.program_id(0)
    steps = pl.num_programs(0)
    width = x_ref.shape[-1]
    plane = lax.axis_index("dp")
    core = lax.rem(lax.axis_index("ty"), 2)

    def loads(i, slot):
        copies = []
        for w, (kind, refs, buf) in enumerate(zip((up_kind, down_kind), srcs, (up_buf, down_buf))):
            if kind is None:
                parts = [(refs[0].at[:, i], buf.at[slot])]
            else:
                half, pair = buf.shape[3], refs[1].shape[0]
                parts = [(refs[0].at[:, i, pl.ds(kind * half, half)], buf.at[slot, :, plane]),
                         (refs[1].at[:, i], buf.at[slot, pl.ds(core * pair, pair), 1 - plane]),
                         (refs[2].at[:, i], buf.at[slot, pl.ds((1 - core) * pair, pair), 1 - plane])]
            copies += [pltpu.make_async_copy(src, dst, sems.at[slot, w, j]) for j, (src, dst) in enumerate(parts)]
        return copies

    slot = lax.rem(step, 2)

    @pl.when(step == 0)
    def _():
        for copy in loads(step, slot):
            copy.start()
        h_ref[...] = norm_rows(x_ref[...].astype(F32), gain_ref[...], shift_ref[...])
        acc_ref[...] = jnp.zeros_like(acc_ref)

    @pl.when(step + 1 < steps)
    def _():
        for copy in loads(step + 1, 1 - slot):
            copy.start()

    for copy in loads(step, slot):
        copy.wait()
    up = up_buf[slot].reshape(width, up_buf.shape[-1])
    down = down_buf[slot].reshape(width, down_buf.shape[-1])
    u = jax.nn.gelu(dot_nn(h_ref[...], up) + bias_ref[0], approximate=True).astype(BF)
    acc_ref[...] += dot_nt(u, down)

    @pl.when(step == steps - 1)
    def _():
        y = x_ref[...].astype(F32) + acc_ref[...] + bd_ref[...]
        if out_ref.shape == x_ref.shape:
            out_ref[...] = y.astype(BF)
        else:
            wl = out_ref.shape[2]
            y_t = y.T.astype(BF)
            for c in range(out_ref.shape[0]):
                for img in range(out_ref.shape[1]):
                    out_ref[c, img] = y_t[c * wl:(c + 1) * wl, img * toks:(img + 1) * toks]


def solution(mesh):
    tx, ty = mesh.shape["tx"], mesh.shape["ty"]
    act_spec = P("dp", None, "tx")
    vec_tx = P(None, "tx")
    proj_spec = P(None, "tx", "ty", None)
    head_vec = P(None, "ty", None)
    in_specs = (act_spec, vec_tx, vec_tx, proj_spec, head_vec, proj_spec, proj_spec, head_vec,
                P(None, "ty", None, "tx"), vec_tx, vec_tx, vec_tx,
                P(None, "tx", "ty"), P(None, "ty"), P(None, "ty", "tx"), vec_tx)

    def local_fn(x_in, ln1_gain, ln1_bias, w_q, b_q, w_k, w_v, b_v, w_o, b_o, ln2_gain, ln2_bias, w_up, b_up, w_down, b_down):
        layers, wl, hl, dim = w_q.shape
        fl = w_up.shape[-1]
        imgs, toks, _ = x_in.shape
        hd = hl * dim
        width = wl * tx
        cols = max(4 * hd, -(-fl // LANES) * LANES)
        per = imgs // ty
        nb = per // tx
        n = nb * toks

        def proj_block(l):
            rows = [w[l].transpose(1, 2, 0).reshape(hd, wl) for w in (w_q, w_k, w_v)] + [w_o[l].reshape(hd, wl)]
            return jnp.pad(jnp.concatenate(rows, axis=0).T, ((0, 0), (0, cols - 4 * hd)))

        def up_block(l):
            return jnp.pad(w_up[l], ((0, 0), (0, cols - fl)))

        def down_block(l):
            return jnp.pad(w_down[l].T, ((0, 0), (0, cols - fl)))

        plane = lax.axis_index("dp")
        core = lax.axis_index("ty") % 2
        half = wl // 2

        def gather(parts):
            rows = sum(p.shape[0] for p in parts)
            full = lax.all_gather(jnp.concatenate(parts, axis=0), ("tx", "ty"), axis=0)
            return full.reshape(tx, ty, rows, cols)

        halves = [("u", 0), ("d", 0), ("u", 1)]
        makers = {"u": up_block, "d": down_block}
        fill = max(0, RING_ROWS - half * len(halves))
        mine = [lax.dynamic_slice_in_dim(makers[kind](l), plane * half, half, axis=0) for kind, l in halves]
        split = gather(mine + [jnp.zeros((fill, cols), BF)])
        both = gather([proj_block(0), proj_block(1)]).reshape(tx, ty, 2, wl, cols)
        last_down = gather([down_block(1)])
        images = lax.dynamic_slice_in_dim(x_in.transpose(0, 2, 1), lax.axis_index("ty") * per, per, axis=0)
        x_t = lax.all_to_all(images, "tx", split_axis=0, concat_axis=0, tiled=True)
        x = x_t.reshape(tx, nb, wl, toks).transpose(1, 3, 0, 2).reshape(n, width)
        on_tx = [ln1_gain, ln1_bias, ln2_gain, ln2_bias, b_o, b_down]
        on_ty = [b_q.reshape(layers, hd), b_v.reshape(layers, hd), b_up]
        vec = lax.all_gather(jnp.concatenate([a.reshape(1, -1) for a in on_tx + on_ty], axis=1), ("tx", "ty"), axis=0)
        vec = vec.reshape(tx, ty, -1)
        at = len(on_tx) * layers * wl
        vt = vec[:, 0, :at].reshape(tx, len(on_tx), layers, wl).transpose(1, 2, 0, 3).reshape(len(on_tx), layers, 1, width)
        vq = vec[0, :, at:at + layers * hd].reshape(ty, layers, hd)
        vv = vec[0, :, at + layers * hd:at + 2 * layers * hd].reshape(ty, layers, hd)
        vu = vec[0, :, at + 2 * layers * hd:].reshape(ty, layers, fl)
        gap = jnp.zeros_like(vq)
        tail = jnp.zeros((ty, layers, cols - 4 * hd), F32)
        bias_a = jnp.concatenate([vq, gap, vv, gap, tail], axis=2).transpose(1, 0, 2).reshape(layers, ty, 1, cols)
        bias_u = jnp.pad(vu, ((0, 0), (0, 0), (0, cols - fl))).transpose(1, 0, 2).reshape(layers, ty, 1, cols)

        swap = [(i, i ^ 1) for i in range(ty)]
        split, x, vt, bias_a, bias_u = lax.optimization_barrier((split, x, vt, bias_a, bias_u))
        got = {}
        for j, key in enumerate(halves):
            sent = lax.dynamic_slice(split, (core * (tx // 2), 0, j * half, 0), (tx // 2, ty, half, cols))
            if j:
                sent, got[halves[0]] = lax.optimization_barrier((sent, got[halves[0]]))
            got[key] = lax.ppermute(sent, "dp", [(0, 1), (1, 0)])
        crossed = {}

        def cross_core(key):
            crossed[key] = (got[key], lax.ppermute(got[key], "ty", swap))

        cross_core(halves[0])

        whole = pl.BlockSpec((n, width), lambda i: (0, 0))
        row = pl.BlockSpec((1, width), lambda i: (0, 0))
        bias = pl.BlockSpec((1, 1, cols), lambda i: (i, 0, 0))
        scratch = [pltpu.VMEM((n, width), BF), pltpu.VMEM((n, width), F32)]
        params = pltpu.CompilerParams(vmem_limit_bytes=VMEM_BYTES, dimension_semantics=("arbitrary",))

        anywhere = pl.BlockSpec(memory_space=pl.ANY)

        for l in range(layers):
            x = pl.pallas_call(
                lambda *refs: attention_kernel(hl, dim, toks, *refs),
                grid=(ty,),
                in_specs=[whole, row, row, bias, row, pl.BlockSpec((tx, 1, 1, wl, cols), lambda i, l=l: (0, i, l, 0, 0))],
                out_specs=whole,
                out_shape=jax.ShapeDtypeStruct((n, width), BF),
                scratch_shapes=scratch,
                compiler_params=params,
                name="attention",
                cost_estimate=pl.CostEstimate(flops=2 * n * width * width * 12, bytes_accessed=2 * width * width * 4, transcendentals=n * toks * 16),
            )(x, vt[0, l], vt[1, l], bias_a[l], vt[4, l], both)
            late = halves[l + 1]
            got[late], x = lax.optimization_barrier((got[late], x))
            cross_core(late)
            last = l == layers - 1
            out = (tx, nb, wl, toks) if last else (n, width)
            kinds, operands, bufs = [], [], []
            for key in (("u", l), ("d", l)):
                if key in crossed:
                    kinds.append(halves.index(key))
                    operands += [split, *crossed[key]]
                    bufs.append(pltpu.VMEM((2, tx, 2, half, cols), BF))
                else:
                    kinds.append(None)
                    operands.append(last_down)
                    bufs.append(pltpu.VMEM((2, tx, wl, cols), BF))
            x = pl.pallas_call(
                lambda *refs, k=tuple(kinds): mlp_kernel(toks, *k, *refs),
                grid=(ty,),
                in_specs=[whole, row, row, bias, row] + [anywhere] * len(operands),
                out_specs=pl.BlockSpec(out, lambda i, r=len(out): (0,) * r),
                out_shape=jax.ShapeDtypeStruct(out, BF),
                scratch_shapes=scratch + bufs + [pltpu.SemaphoreType.DMA((2, 2, 3))],
                compiler_params=params,
                name="mlp",
                cost_estimate=pl.CostEstimate(flops=2 * n * width * cols * ty * 4, bytes_accessed=4 * width * cols * ty, transcendentals=n * cols * ty),
            )(x, vt[2, l], vt[3, l], bias_u[l], vt[5, l], *operands)
        y = lax.all_to_all(x.reshape(tx * nb, wl, toks), "tx", split_axis=0, concat_axis=0, tiled=True)
        y = lax.all_gather(y, "ty", axis=0, tiled=True)
        return y.transpose(0, 2, 1)

    return jax.shard_map(local_fn, mesh=mesh, in_specs=in_specs, out_specs=act_spec, check_vma=False)
```

```python
import jax
import jax.numpy as jnp
from jax import lax
from jax.experimental import pallas as pl
from jax.experimental.pallas import tpu as pltpu
from jax.sharding import PartitionSpec as P


EPS = 1e-6
BF = jnp.bfloat16
F32 = jnp.float32
LANES = 128
VMEM_BYTES = 60 * 1024 * 1024


def norm_rows(x_f, gain, shift):
    mean = jnp.mean(x_f, axis=-1, keepdims=True)
    centred = x_f - mean
    variance = jnp.mean(centred * centred, axis=-1, keepdims=True)
    return (centred * lax.rsqrt(variance + EPS) * gain + shift).astype(BF)


def dot_nn(a, b):
    return lax.dot_general(a, b, (((1,), (0,)), ((), ())), preferred_element_type=F32)


def dot_nt(a, b):
    return lax.dot_general(a, b, (((1,), (1,)), ((), ())), preferred_element_type=F32)


def attention_kernel(heads, dim, toks, x_ref, gain_ref, shift_ref, bias_ref, bo_ref, w_ref, out_ref, h_ref, acc_ref):
    step = pl.program_id(0)
    width = x_ref.shape[-1]
    hd = heads * dim
    span = -(-hd // LANES) * LANES

    @pl.when(step == 0)
    def _():
        h_ref[...] = norm_rows(x_ref[...].astype(F32), gain_ref[...], shift_ref[...])
        acc_ref[...] = jnp.zeros_like(acc_ref)

    w = w_ref[...].reshape(width, w_ref.shape[-1])
    cols = w.shape[-1]
    qkv = dot_nn(h_ref[...], w) + bias_ref[0]
    q_f = qkv[:, :span]
    k = pltpu.roll(qkv, cols - hd, 1)[:, :span].astype(BF)
    v = pltpu.roll(qkv, hd, 1)[:, cols - span:].astype(BF)
    lane = lax.broadcasted_iota(jnp.int32, (toks, span), 1)
    outs = []
    for img in range(x_ref.shape[0] // toks):
        rows = slice(img * toks, (img + 1) * toks)
        q_i, k_i, v_i = q_f[rows], k[rows], v[rows]
        o_i = jnp.zeros((toks, span), F32)
        for head in range(heads):
            q_h = jnp.where((lane >= head * dim) & (lane < (head + 1) * dim), q_i, 0.0).astype(BF)
            s = dot_nt(q_h, k_i) * (dim ** -0.5)
            e = jnp.exp(s - jnp.max(s, axis=-1, keepdims=True))
            p = (e / jnp.sum(e, axis=-1, keepdims=True)).astype(BF)
            lo = span - hd + head * dim
            o_i = jnp.where((lane >= lo) & (lane < lo + dim), dot_nn(p, v_i), o_i)
        outs.append(o_i)
    acc_ref[...] += dot_nt(jnp.concatenate(outs, axis=0).astype(BF), w[:, cols - span:])

    @pl.when(step == pl.num_programs(0) - 1)
    def _():
        out_ref[...] = (x_ref[...].astype(F32) + acc_ref[...] + bo_ref[...]).astype(BF)


def load_ahead(loads, first=lambda: None):
    step = pl.program_id(0)
    slot = lax.rem(step, 2)

    @pl.when(step == 0)
    def _():
        for copy in loads(step, slot):
            copy.start()
        first()

    @pl.when(step + 1 < pl.num_programs(0))
    def _():
        for copy in loads(step + 1, 1 - slot):
            copy.start()

    for copy in loads(step, slot):
        copy.wait()
    return slot


def half_loads(srcs, bufs, sems):
    plane = lax.axis_index("dp")
    core = lax.rem(lax.axis_index("ty"), 2)

    def loads(i, slot):
        copies = []
        for w, buf in enumerate(bufs):
            own, same, other = srcs[3 * w:3 * w + 3]
            pair = same.shape[0]
            parts = [(own.at[:, i], buf.at[slot, :, plane]),
                     (same.at[:, i], buf.at[slot, pl.ds(core * pair, pair), 1 - plane]),
                     (other.at[:, i], buf.at[slot, pl.ds((1 - core) * pair, pair), 1 - plane])]
            copies += [pltpu.make_async_copy(src, dst, sems.at[slot, w, j]) for j, (src, dst) in enumerate(parts)]
        return copies

    return loads


def mlp_kernel(x_ref, gain_ref, shift_ref, bias_ref, bd_ref, u0, u1, u2, d0, d1, d2, out_ref, h_ref, acc_ref, up_buf, down_buf, sems):
    step = pl.program_id(0)
    width = x_ref.shape[-1]

    def first():
        h_ref[...] = norm_rows(x_ref[...].astype(F32), gain_ref[...], shift_ref[...])
        acc_ref[...] = jnp.zeros_like(acc_ref)

    slot = load_ahead(half_loads((u0, u1, u2, d0, d1, d2), (up_buf, down_buf), sems), first)
    up = up_buf[slot].reshape(width, up_buf.shape[-1])
    down = down_buf[slot].reshape(width, down_buf.shape[-1])
    u = jax.nn.gelu(dot_nn(h_ref[...], up) + bias_ref[0], approximate=True).astype(BF)
    acc_ref[...] += dot_nt(u, down)

    @pl.when(step == pl.num_programs(0) - 1)
    def _():
        out_ref[...] = (x_ref[...].astype(F32) + acc_ref[...] + bd_ref[...]).astype(BF)


def up_kernel(x_ref, gain_ref, shift_ref, bias_ref, u0, u1, u2, out_ref, h_ref, up_buf, sems):
    width = x_ref.shape[-1]

    def first():
        h_ref[...] = norm_rows(x_ref[...].astype(F32), gain_ref[...], shift_ref[...])

    slot = load_ahead(half_loads((u0, u1, u2), (up_buf,), sems), first)
    up = up_buf[slot].reshape(width, up_buf.shape[-1])
    out_ref[0] = jax.nn.gelu(dot_nn(h_ref[...], up) + bias_ref[0], approximate=True).astype(BF)


def down_kernel(order, toks, x_ref, bd_ref, u_ref, down_ref, out_ref, acc_ref):
    step = pl.program_id(0)
    width = x_ref.shape[-1]

    @pl.when(step == 0)
    def _():
        acc_ref[...] = x_ref[...].astype(F32) + bd_ref[...]

    acc_ref[...] += dot_nt(u_ref[0], down_ref[...].reshape(width, down_ref.shape[-1]))

    @pl.when(step == pl.num_programs(0) - 1)
    def _():
        wl = out_ref.shape[2]
        y_t = acc_ref[...].T.astype(BF)
        for i, block in enumerate(order):
            for img in range(out_ref.shape[1]):
                out_ref[block, img] = y_t[i * wl:(i + 1) * wl, img * toks:(img + 1) * toks]


def solution(mesh):
    tx, ty = mesh.shape["tx"], mesh.shape["ty"]
    act_spec = P("dp", None, "tx")
    vec_tx = P(None, "tx")
    proj_spec = P(None, "tx", "ty", None)
    head_vec = P(None, "ty", None)
    in_specs = (act_spec, vec_tx, vec_tx, proj_spec, head_vec, proj_spec, proj_spec, head_vec,
                P(None, "ty", None, "tx"), vec_tx, vec_tx, vec_tx,
                P(None, "tx", "ty"), P(None, "ty"), P(None, "ty", "tx"), vec_tx)

    def local_fn(x_in, ln1_gain, ln1_bias, w_q, b_q, w_k, w_v, b_v, w_o, b_o, ln2_gain, ln2_bias, w_up, b_up, w_down, b_down):
        layers, wl, hl, dim = w_q.shape
        fl = w_up.shape[-1]
        imgs, toks, _ = x_in.shape
        hd = hl * dim
        width = wl * tx
        cols = max(4 * hd, -(-fl // LANES) * LANES)
        per = imgs // ty
        nb = per // tx
        n = nb * toks

        def proj_block(l):
            rows = [w[l].transpose(1, 2, 0).reshape(hd, wl) for w in (w_q, w_k, w_v)] + [w_o[l].reshape(hd, wl)]
            return jnp.pad(jnp.concatenate(rows, axis=0).T, ((0, 0), (0, cols - 4 * hd)))

        def up_block(l):
            return jnp.pad(w_up[l], ((0, 0), (0, cols - fl)))

        def down_block(l):
            return jnp.pad(w_down[l].T, ((0, 0), (0, cols - fl)))

        plane = lax.axis_index("dp")
        core = lax.axis_index("ty") % 2
        half = wl // 2

        order = [1, 0] + list(range(2, tx))
        groups = [[t * ty + i for t in order for i in range(ty)]]

        def blocks(a):
            return jnp.concatenate([a[i:i + 1] for i in order], axis=0)

        def gather(block):
            full = lax.all_gather(block, ("tx", "ty"), axis=0, axis_index_groups=groups)
            return full.reshape(tx, ty, *block.shape)

        halves = [("u", 0), ("d", 0), ("u", 1)]
        makers = {"u": up_block, "d": down_block}
        split = {(kind, l): gather(lax.dynamic_slice_in_dim(makers[kind](l), plane * half, half, axis=0)) for kind, l in halves}
        proj = [gather(proj_block(0)), gather(proj_block(1))]
        last_down = gather(down_block(1))

        images = lax.dynamic_slice_in_dim(x_in.transpose(0, 2, 1), lax.axis_index("ty") * per, per, axis=0)
        x_t = lax.all_to_all(images, "tx", split_axis=0, concat_axis=0, tiled=True)
        x = blocks(x_t.reshape(tx, nb, wl, toks)).transpose(1, 3, 0, 2).reshape(n, width)
        swap = [(i, i ^ 1) for i in range(ty)]
        got, crossed = {}, {}

        def to_send(key):
            return lax.dynamic_slice_in_dim(split[key], core * (tx // 2), tx // 2, axis=0)

        def cross_plane(key, sent):
            got[key] = lax.ppermute(sent, "dp", [(0, 1), (1, 0)])

        def cross_core(key):
            crossed[key] = (got[key], lax.ppermute(got[key], "ty", swap))

        split[halves[0]], x = lax.optimization_barrier((split[halves[0]], x))
        on_tx = [ln1_gain, ln1_bias, ln2_gain, ln2_bias, b_o, b_down]
        on_ty = [b_q.reshape(layers, hd), b_v.reshape(layers, hd), b_up]
        own = jnp.concatenate([a.reshape(1, -1) for a in on_tx + on_ty], axis=1)
        own, sent = lax.optimization_barrier((own, to_send(halves[0])))
        vec = lax.all_gather(own, ("tx", "ty"), axis=0)
        vec = blocks(vec.reshape(tx, ty, -1))
        at = len(on_tx) * layers * wl
        vt = vec[:, 0, :at].reshape(tx, len(on_tx), layers, wl).transpose(1, 2, 0, 3).reshape(len(on_tx), layers, 1, width)
        vq = vec[0, :, at:at + layers * hd].reshape(ty, layers, hd)
        vv = vec[0, :, at + layers * hd:at + 2 * layers * hd].reshape(ty, layers, hd)
        vu = vec[0, :, at + 2 * layers * hd:].reshape(ty, layers, fl)
        gap = jnp.zeros_like(vq)
        tail = jnp.zeros((ty, layers, cols - 4 * hd), F32)
        bias_a = jnp.concatenate([vq, gap, vv, gap, tail], axis=2).transpose(1, 0, 2).reshape(layers, ty, 1, cols)
        bias_u = jnp.pad(vu, ((0, 0), (0, 0), (0, cols - fl))).transpose(1, 0, 2).reshape(layers, ty, 1, cols)

        cross_plane(halves[0], sent)
        for key in halves[1:]:
            split[key], vec = lax.optimization_barrier((split[key], vec))
            cross_plane(key, to_send(key))
        cross_core(halves[0])

        whole = pl.BlockSpec((n, width), lambda i: (0, 0))
        row = pl.BlockSpec((1, width), lambda i: (0, 0))
        bias = pl.BlockSpec((1, 1, cols), lambda i: (i, 0, 0))
        scratch = [pltpu.VMEM((n, width), BF), pltpu.VMEM((n, width), F32)]
        params = pltpu.CompilerParams(vmem_limit_bytes=VMEM_BYTES, dimension_semantics=("arbitrary",))

        anywhere = pl.BlockSpec(memory_space=pl.ANY)
        rows_bf, rows_f = scratch
        half_buf = pltpu.VMEM((2, tx, 2, half, cols), BF)
        act = jax.ShapeDtypeStruct((n, width), BF)
        dot_flops = 2 * n * width * cols * ty

        def kernel(fn, in_specs, out_spec, out_shape, scratch_shapes, flops):
            return pl.pallas_call(fn, grid=(ty,), in_specs=in_specs, out_specs=out_spec, out_shape=out_shape,
                                  scratch_shapes=scratch_shapes, compiler_params=params,
                                  cost_estimate=pl.CostEstimate(flops=flops, bytes_accessed=width * cols * ty * 4, transcendentals=n * cols * ty))

        for l in range(layers):
            x = kernel(lambda *refs: attention_kernel(hl, dim, toks, *refs),
                       [whole, row, row, bias, row, pl.BlockSpec((tx, 1, wl, cols), lambda i: (0, i, 0, 0))],
                       whole, act, scratch, 4 * dot_flops)(x, vt[0, l], vt[1, l], bias_a[l], vt[4, l], proj[l])
            late = halves[l + 1]
            got[late], x = lax.optimization_barrier((got[late], x))
            cross_core(late)
            up = (split["u", l], *crossed["u", l])
            if l < layers - 1:
                down = (split["d", l], *crossed["d", l])
                x = kernel(mlp_kernel, [whole, row, row, bias, row] + [anywhere] * 6, whole, act,
                           scratch + [half_buf, half_buf, pltpu.SemaphoreType.DMA((2, 2, 3))], 4 * dot_flops,
                           )(x, vt[2, l], vt[3, l], bias_u[l], vt[5, l], *up, *down)
            else:
                hidden = pl.BlockSpec((1, n, cols), lambda i: (i, 0, 0))
                u = kernel(up_kernel, [whole, row, row, bias] + [anywhere] * 3, hidden,
                           jax.ShapeDtypeStruct((ty, n, cols), BF), [rows_bf, half_buf, pltpu.SemaphoreType.DMA((2, 1, 3))],
                           2 * dot_flops)(x, vt[2, l], vt[3, l], bias_u[l], *up)
                out = (tx, nb, wl, toks)
                x = kernel(lambda *refs: down_kernel(order, toks, *refs),
                           [whole, row, hidden, pl.BlockSpec((tx, 1, wl, cols), lambda i: (0, i, 0, 0))],
                           pl.BlockSpec(out, lambda i: (0, 0, 0, 0)), jax.ShapeDtypeStruct(out, BF), [rows_f],
                           2 * dot_flops)(x, vt[5, l], u, last_down)
        y = lax.all_to_all(x.reshape(tx * nb, wl, toks), "tx", split_axis=0, concat_axis=0, tiled=True)
        y = lax.all_gather(y, "ty", axis=0, tiled=True)
        return y.transpose(0, 2, 1)

    return jax.shard_map(local_fn, mesh=mesh, in_specs=in_specs, out_specs=act_spec, check_vma=False)
```

```python
import jax
import jax.numpy as jnp
from jax import lax
from jax.experimental import pallas as pl
from jax.experimental.pallas import tpu as pltpu
from jax.sharding import PartitionSpec as P


EPS = 1e-6
BF = jnp.bfloat16
F32 = jnp.float32
LANES = 128
VMEM_BYTES = 60 * 1024 * 1024


def norm_rows(x_f, gain, shift):
    mean = jnp.mean(x_f, axis=-1, keepdims=True)
    centred = x_f - mean
    variance = jnp.mean(centred * centred, axis=-1, keepdims=True)
    return (centred * lax.rsqrt(variance + EPS) * gain + shift).astype(BF)


def dot_nn(a, b):
    return lax.dot_general(a, b, (((1,), (0,)), ((), ())), preferred_element_type=F32)


def dot_nt(a, b):
    return lax.dot_general(a, b, (((1,), (1,)), ((), ())), preferred_element_type=F32)


def attention_kernel(heads, dim, toks, x_ref, gain_ref, shift_ref, bias_ref, bo_ref, w_ref, out_ref, h_ref, acc_ref):
    step = pl.program_id(0)
    width = x_ref.shape[-1]
    hd = heads * dim
    span = -(-hd // LANES) * LANES

    @pl.when(step == 0)
    def _():
        h_ref[...] = norm_rows(x_ref[...].astype(F32), gain_ref[...], shift_ref[...])
        acc_ref[...] = jnp.zeros_like(acc_ref)

    w = w_ref[...].reshape(width, w_ref.shape[-1])
    cols = w.shape[-1]
    qkv = dot_nn(h_ref[...], w) + bias_ref[0]
    q_f = qkv[:, :span]
    k = pltpu.roll(qkv, cols - hd, 1)[:, :span].astype(BF)
    v = pltpu.roll(qkv, hd, 1)[:, cols - span:].astype(BF)
    lane = lax.broadcasted_iota(jnp.int32, (toks, span), 1)
    outs = []
    for img in range(x_ref.shape[0] // toks):
        rows = slice(img * toks, (img + 1) * toks)
        q_i, k_i, v_i = q_f[rows], k[rows], v[rows]
        o_i = jnp.zeros((toks, span), F32)
        for head in range(heads):
            q_h = jnp.where((lane >= head * dim) & (lane < (head + 1) * dim), q_i, 0.0).astype(BF)
            s = dot_nt(q_h, k_i) * (dim ** -0.5)
            e = jnp.exp(s - jnp.max(s, axis=-1, keepdims=True))
            p = (e / jnp.sum(e, axis=-1, keepdims=True)).astype(BF)
            lo = span - hd + head * dim
            o_i = jnp.where((lane >= lo) & (lane < lo + dim), dot_nn(p, v_i), o_i)
        outs.append(o_i)
    acc_ref[...] += dot_nt(jnp.concatenate(outs, axis=0).astype(BF), w[:, cols - span:])

    @pl.when(step == pl.num_programs(0) - 1)
    def _():
        out_ref[...] = (x_ref[...].astype(F32) + acc_ref[...] + bo_ref[...]).astype(BF)


def load_ahead(loads, first=lambda: None):
    step = pl.program_id(0)
    slot = lax.rem(step, 2)

    @pl.when(step == 0)
    def _():
        for copy in loads(step, slot):
            copy.start()
        first()

    @pl.when(step + 1 < pl.num_programs(0))
    def _():
        for copy in loads(step + 1, 1 - slot):
            copy.start()

    for copy in loads(step, slot):
        copy.wait()
    return slot


def half_loads(offsets, srcs, bufs, sems):
    plane = lax.axis_index("dp")
    core = lax.rem(lax.axis_index("ty"), 2)

    def loads(i, slot):
        copies = []
        for w, buf in enumerate(bufs):
            own, same, other = srcs[3 * w:3 * w + 3]
            pair = same.shape[0]
            parts = [(own.at[:, i, pl.ds(offsets[w], buf.shape[3])], buf.at[slot, :, plane]),
                     (same.at[:, i], buf.at[slot, pl.ds(core * pair, pair), 1 - plane]),
                     (other.at[:, i], buf.at[slot, pl.ds((1 - core) * pair, pair), 1 - plane])]
            copies += [pltpu.make_async_copy(src, dst, sems.at[slot, w, j]) for j, (src, dst) in enumerate(parts)]
        return copies

    return loads


def mlp_kernel(offsets, x_ref, gain_ref, shift_ref, bias_ref, bd_ref, u0, u1, u2, d0, d1, d2, out_ref, h_ref, acc_ref, up_buf, down_buf, sems):
    step = pl.program_id(0)
    width = x_ref.shape[-1]

    def first():
        h_ref[...] = norm_rows(x_ref[...].astype(F32), gain_ref[...], shift_ref[...])
        acc_ref[...] = jnp.zeros_like(acc_ref)

    slot = load_ahead(half_loads(offsets, (u0, u1, u2, d0, d1, d2), (up_buf, down_buf), sems), first)
    up = up_buf[slot].reshape(width, up_buf.shape[-1])
    down = down_buf[slot].reshape(width, down_buf.shape[-1])
    u = jax.nn.gelu(dot_nn(h_ref[...], up) + bias_ref[0], approximate=True).astype(BF)
    acc_ref[...] += dot_nt(u, down)

    @pl.when(step == pl.num_programs(0) - 1)
    def _():
        out_ref[...] = (x_ref[...].astype(F32) + acc_ref[...] + bd_ref[...]).astype(BF)


def up_kernel(offsets, x_ref, gain_ref, shift_ref, bias_ref, u0, u1, u2, out_ref, h_ref, up_buf, sems):
    width = x_ref.shape[-1]

    def first():
        h_ref[...] = norm_rows(x_ref[...].astype(F32), gain_ref[...], shift_ref[...])

    slot = load_ahead(half_loads(offsets, (u0, u1, u2), (up_buf,), sems), first)
    up = up_buf[slot].reshape(width, up_buf.shape[-1])
    out_ref[0] = jax.nn.gelu(dot_nn(h_ref[...], up) + bias_ref[0], approximate=True).astype(BF)


def down_kernel(order, x_ref, bd_ref, u_ref, down_ref, out_ref, acc_ref):
    step = pl.program_id(0)
    width = x_ref.shape[-1]

    @pl.when(step == 0)
    def _():
        acc_ref[...] = x_ref[...].astype(F32) + bd_ref[...]

    acc_ref[...] += dot_nt(u_ref[0], down_ref[...].reshape(width, down_ref.shape[-1]))

    @pl.when(step == pl.num_programs(0) - 1)
    def _():
        wl = out_ref.shape[1]
        y_t = acc_ref[...].T.astype(BF)
        for i, block in enumerate(order):
            out_ref[block] = y_t[i * wl:(i + 1) * wl]


def place_kernel(tx, ty, per, nb, *refs):
    *srcs, out_ref, sems = refs
    t, y = lax.axis_index("tx"), lax.axis_index("ty")
    copies = []
    for j, src in enumerate(srcs):
        img, dist = divmod(j, ty)
        group = y + dist - 2 * sum(bit * lax.rem(y // bit, 2) for bit in (1, 2) if dist & bit)
        for k in range(tx):
            index = group * per + lax.rem(t - k + tx, tx) * nb + img
            copies.append(pltpu.make_async_copy(src.at[k], out_ref.at[index], sems.at[j, k]))
    for copy in copies:
        copy.start()
    for copy in copies:
        copy.wait()


def solution(mesh):
    tx, ty = mesh.shape["tx"], mesh.shape["ty"]
    act_spec = P("dp", None, "tx")
    vec_tx = P(None, "tx")
    proj_spec = P(None, "tx", "ty", None)
    head_vec = P(None, "ty", None)
    in_specs = (act_spec, vec_tx, vec_tx, proj_spec, head_vec, proj_spec, proj_spec, head_vec,
                P(None, "ty", None, "tx"), vec_tx, vec_tx, vec_tx,
                P(None, "tx", "ty"), P(None, "ty"), P(None, "ty", "tx"), vec_tx)

    def local_fn(x_in, ln1_gain, ln1_bias, w_q, b_q, w_k, w_v, b_v, w_o, b_o, ln2_gain, ln2_bias, w_up, b_up, w_down, b_down):
        layers, wl, hl, dim = w_q.shape
        fl = w_up.shape[-1]
        imgs, toks, _ = x_in.shape
        hd = hl * dim
        width = wl * tx
        cols = max(4 * hd, -(-fl // LANES) * LANES)
        per = imgs // ty
        nb = per // tx
        n = nb * toks

        def proj_block(l):
            rows = [w[l].transpose(1, 2, 0).reshape(hd, wl) for w in (w_q, w_k, w_v)] + [w_o[l].reshape(hd, wl)]
            return jnp.pad(jnp.concatenate(rows, axis=0).T, ((0, 0), (0, cols - 4 * hd)))

        def up_block(l):
            return jnp.pad(w_up[l], ((0, 0), (0, cols - fl)))

        def down_block(l):
            return jnp.pad(w_down[l].T, ((0, 0), (0, cols - fl)))

        plane = lax.axis_index("dp")
        core = lax.axis_index("ty") % 2
        half = wl // 2

        order = [1, 0] + list(range(2, tx))
        groups = [[t * ty + i for t in order for i in range(ty)]]

        def blocks(a):
            return jnp.concatenate([a[i:i + 1] for i in order], axis=0)

        def gather(block):
            full = lax.all_gather(block, ("tx", "ty"), axis=0, axis_index_groups=groups)
            return full.reshape(tx, ty, *block.shape)

        halves = [("u", 0), ("d", 0), ("u", 1)]

        def half_block(block):
            return lax.dynamic_slice_in_dim(block, plane * half, half, axis=0)

        first = gather(jnp.concatenate([half_block(up_block(0)), half_block(down_block(0))], axis=0))
        second = gather(jnp.concatenate([proj_block(0), half_block(up_block(1))], axis=0))
        third = gather(proj_block(1))
        last_down = gather(down_block(1))
        proj = [second, third]
        split = {("u", 0): (first, 0), ("d", 0): (first, half), ("u", 1): (second, wl)}

        images = lax.dynamic_slice_in_dim(x_in.transpose(0, 2, 1), lax.axis_index("ty") * per, per, axis=0)
        x_t = lax.all_to_all(images, "tx", split_axis=0, concat_axis=0, tiled=True)
        x = blocks(x_t.reshape(tx, nb, wl, toks)).transpose(1, 3, 0, 2).reshape(n, width)
        swap = [(i, i ^ 1) for i in range(ty)]
        got, crossed = {}, {}

        def to_send(key):
            full, at = split[key]
            return lax.dynamic_slice(full, (core * (tx // 2), 0, at, 0), (tx // 2, ty, half, cols))

        def cross_plane(key, sent):
            got[key] = lax.ppermute(sent, "dp", [(0, 1), (1, 0)])

        def cross_core(key):
            crossed[key] = (got[key], lax.ppermute(got[key], "ty", swap))

        first, x = lax.optimization_barrier((first, x))
        split["u", 0] = (first, 0)
        on_tx = [ln1_gain, ln1_bias, ln2_gain, ln2_bias, b_o, b_down]
        on_ty = [b_q.reshape(layers, hd), b_v.reshape(layers, hd), b_up]
        own = jnp.concatenate([a.reshape(1, -1) for a in on_tx + on_ty], axis=1)
        own, sent = lax.optimization_barrier((own, to_send(halves[0])))
        vec = lax.all_gather(own, ("tx", "ty"), axis=0)
        vec = blocks(vec.reshape(tx, ty, -1))
        at = len(on_tx) * layers * wl
        vt = vec[:, 0, :at].reshape(tx, len(on_tx), layers, wl).transpose(1, 2, 0, 3).reshape(len(on_tx), layers, 1, width)
        vq = vec[0, :, at:at + layers * hd].reshape(ty, layers, hd)
        vv = vec[0, :, at + layers * hd:at + 2 * layers * hd].reshape(ty, layers, hd)
        vu = vec[0, :, at + 2 * layers * hd:].reshape(ty, layers, fl)
        gap = jnp.zeros_like(vq)
        tail = jnp.zeros((ty, layers, cols - 4 * hd), F32)
        bias_a = jnp.concatenate([vq, gap, vv, gap, tail], axis=2).transpose(1, 0, 2).reshape(layers, ty, 1, cols)
        bias_u = jnp.pad(vu, ((0, 0), (0, 0), (0, cols - fl))).transpose(1, 0, 2).reshape(layers, ty, 1, cols)

        cross_plane(halves[0], sent)
        for key in halves[1:]:
            sent, vec = lax.optimization_barrier((to_send(key), vec))
            cross_plane(key, sent)
        cross_core(halves[0])

        whole = pl.BlockSpec((n, width), lambda i: (0, 0))
        row = pl.BlockSpec((1, width), lambda i: (0, 0))
        bias = pl.BlockSpec((1, 1, cols), lambda i: (i, 0, 0))
        scratch = [pltpu.VMEM((n, width), BF), pltpu.VMEM((n, width), F32)]
        params = pltpu.CompilerParams(vmem_limit_bytes=VMEM_BYTES, dimension_semantics=("arbitrary",))

        anywhere = pl.BlockSpec(memory_space=pl.ANY)
        rows_bf, _ = scratch
        half_buf = pltpu.VMEM((2, tx, 2, half, cols), BF)
        act = jax.ShapeDtypeStruct((n, width), BF)
        dot_flops = 2 * n * width * cols * ty

        def kernel(fn, in_specs, out_spec, out_shape, scratch_shapes, flops):
            return pl.pallas_call(fn, grid=(ty,), in_specs=in_specs, out_specs=out_spec, out_shape=out_shape,
                                  scratch_shapes=scratch_shapes, compiler_params=params,
                                  cost_estimate=pl.CostEstimate(flops=flops, bytes_accessed=width * cols * ty * 4, transcendentals=n * cols * ty))

        for l in range(layers):
            x = kernel(lambda *refs: attention_kernel(hl, dim, toks, *refs),
                       [whole, row, row, bias, row, pl.BlockSpec((tx, 1, wl, cols), lambda i: (0, i, 0, 0))],
                       whole, act, scratch, 4 * dot_flops)(x, vt[0, l], vt[1, l], bias_a[l], vt[4, l], proj[l])
            late = halves[l + 1]
            got[late], x = lax.optimization_barrier((got[late], x))
            cross_core(late)
            up = (split["u", l][0], *crossed["u", l])
            if l < layers - 1:
                down = (split["d", l][0], *crossed["d", l])
                offsets = (split["u", l][1], split["d", l][1])
                x = kernel(lambda *refs, o=offsets: mlp_kernel(o, *refs), [whole, row, row, bias, row] + [anywhere] * 6, whole, act,
                           scratch + [half_buf, half_buf, pltpu.SemaphoreType.DMA((2, 2, 3))], 4 * dot_flops,
                           )(x, vt[2, l], vt[3, l], bias_u[l], vt[5, l], *up, *down)
            else:
                hidden = pl.BlockSpec((1, n, cols), lambda i: (i, 0, 0))
                u = kernel(lambda *refs, o=(split["u", l][1],): up_kernel(o, *refs), [whole, row, row, bias] + [anywhere] * 3, hidden,
                           jax.ShapeDtypeStruct((ty, n, cols), BF), [rows_bf, half_buf, pltpu.SemaphoreType.DMA((2, 1, 3))],
                           2 * dot_flops)(x, vt[2, l], vt[3, l], bias_u[l], *up)
                outs = []
                for img in range(nb):
                    outs.append(kernel(lambda *refs: down_kernel(order, *refs),
                                       [pl.BlockSpec((toks, width), lambda i, m=img: (m, 0)), row,
                                        pl.BlockSpec((1, toks, cols), lambda i, m=img: (i, m, 0)),
                                        pl.BlockSpec((tx, 1, wl, cols), lambda i: (0, i, 0, 0))],
                                       pl.BlockSpec((tx, wl, toks), lambda i: (0, 0, 0)),
                                       jax.ShapeDtypeStruct((tx, wl, toks), BF), [pltpu.VMEM((toks, width), F32)],
                                       2 * dot_flops // nb)(x, vt[5, l], u, last_down))
        me = lax.axis_index("tx")
        pieces = []
        for y_i in outs:
            moved = []
            for k in range(tx):
                part = lax.dynamic_index_in_dim(y_i, (me + k) % tx, keepdims=False)
                moved.append(lax.ppermute(part, "tx", [(i, (i + k) % tx) for i in range(tx)]) if k else part)
            by_group = [jnp.stack(moved)]
            for dist in range(1, ty):
                bit = dist & -dist
                by_group.append(lax.ppermute(by_group[dist - bit], "ty", [(i, i ^ bit) for i in range(ty)]))
            pieces += by_group
        y = pl.pallas_call(lambda *refs: place_kernel(tx, ty, per, nb, *refs),
                           in_specs=[pl.BlockSpec(memory_space=pltpu.VMEM)] * len(pieces),
                           out_specs=pl.BlockSpec(memory_space=pl.ANY),
                           out_shape=jax.ShapeDtypeStruct((imgs, wl, toks), BF),
                           scratch_shapes=[pltpu.SemaphoreType.DMA((len(pieces), tx))],
                           compiler_params=pltpu.CompilerParams(vmem_limit_bytes=VMEM_BYTES // 2), name="place")(*pieces)
        return y.transpose(0, 2, 1)

    return jax.shard_map(local_fn, mesh=mesh, in_specs=in_specs, out_specs=act_spec, check_vma=False)
```

```python
import jax
import jax.numpy as jnp
from jax import lax
from jax.experimental import pallas as pl
from jax.experimental.pallas import tpu as pltpu
from jax.sharding import PartitionSpec as P


EPS = 1e-6
BF = jnp.bfloat16
F32 = jnp.float32
LANES = 128
VMEM_BYTES = 60 * 1024 * 1024


def norm_rows(x_f, gain, shift):
    mean = jnp.mean(x_f, axis=-1, keepdims=True)
    centred = x_f - mean
    variance = jnp.mean(centred * centred, axis=-1, keepdims=True)
    return (centred * lax.rsqrt(variance + EPS) * gain + shift).astype(BF)


def dot_nn(a, b):
    return lax.dot_general(a, b, (((1,), (0,)), ((), ())), preferred_element_type=F32)


def dot_nt(a, b):
    return lax.dot_general(a, b, (((1,), (1,)), ((), ())), preferred_element_type=F32)


def attention_kernel(heads, dim, toks, x_ref, gain_ref, shift_ref, bias_ref, bo_ref, w_ref, out_ref, h_ref, acc_ref):
    step = pl.program_id(0)
    width = x_ref.shape[-1]
    hd = heads * dim
    span = -(-hd // LANES) * LANES

    @pl.when(step == 0)
    def _():
        h_ref[...] = norm_rows(x_ref[...].astype(F32), gain_ref[...], shift_ref[...])
        acc_ref[...] = jnp.zeros_like(acc_ref)

    w = w_ref[...].reshape(width, w_ref.shape[-1])
    cols = w.shape[-1]
    qkv = dot_nn(h_ref[...], w) + bias_ref[0]
    q_f = qkv[:, :span]
    k = pltpu.roll(qkv, cols - hd, 1)[:, :span].astype(BF)
    v = pltpu.roll(qkv, hd, 1)[:, cols - span:].astype(BF)
    lane = lax.broadcasted_iota(jnp.int32, (toks, span), 1)
    outs = []
    for img in range(x_ref.shape[0] // toks):
        rows = slice(img * toks, (img + 1) * toks)
        q_i, k_i, v_i = q_f[rows], k[rows], v[rows]
        o_i = jnp.zeros((toks, span), F32)
        for head in range(heads):
            q_h = jnp.where((lane >= head * dim) & (lane < (head + 1) * dim), q_i, 0.0).astype(BF)
            s = dot_nt(q_h, k_i) * (dim ** -0.5)
            e = jnp.exp(s - jnp.max(s, axis=-1, keepdims=True))
            p = (e / jnp.sum(e, axis=-1, keepdims=True)).astype(BF)
            lo = span - hd + head * dim
            o_i = jnp.where((lane >= lo) & (lane < lo + dim), dot_nn(p, v_i), o_i)
        outs.append(o_i)
    acc_ref[...] += dot_nt(jnp.concatenate(outs, axis=0).astype(BF), w[:, cols - span:])

    @pl.when(step == pl.num_programs(0) - 1)
    def _():
        out_ref[...] = (x_ref[...].astype(F32) + acc_ref[...] + bo_ref[...]).astype(BF)


def load_ahead(loads, first=lambda: None):
    step = pl.program_id(0)
    slot = lax.rem(step, 2)

    @pl.when(step == 0)
    def _():
        for copy in loads(step, slot):
            copy.start()
        first()

    @pl.when(step + 1 < pl.num_programs(0))
    def _():
        for copy in loads(step + 1, 1 - slot):
            copy.start()

    for copy in loads(step, slot):
        copy.wait()
    return slot


def half_loads(offsets, srcs, bufs, sems):
    plane = lax.axis_index("dp")
    core = lax.rem(lax.axis_index("ty"), 2)
    per = len(srcs) // len(bufs)

    def loads(i, slot):
        copies = []
        for w, buf in enumerate(bufs):
            own, same, other, *rest = srcs[per * w:per * (w + 1)]
            pair, size = same.shape[0], same.shape[2]
            mine = pl.ds(pl.multiple_of(plane * size, 16), size)
            theirs = pl.ds(pl.multiple_of((1 - plane) * size, 16), size)
            parts = [(own.at[:, i, pl.ds(offsets[w], size)], buf.at[slot, :, mine]),
                     (same.at[:, i], buf.at[slot, pl.ds(core * pair, pair), theirs]),
                     (other.at[:, i], buf.at[slot, pl.ds((1 - core) * pair, pair), theirs])]
            parts += [(r.at[:, i], buf.at[slot, :, pl.ds(2 * size, r.shape[2])]) for r in rest]
            copies += [pltpu.make_async_copy(src, dst, sems.at[slot, w, j]) for j, (src, dst) in enumerate(parts)]
        return copies

    return loads


def mlp_kernel(offsets, x_ref, gain_ref, shift_ref, bias_ref, bd_ref, u0, u1, u2, d0, d1, d2, out_ref, h_ref, acc_ref, up_buf, down_buf, sems):
    step = pl.program_id(0)
    width = x_ref.shape[-1]

    def first():
        h_ref[...] = norm_rows(x_ref[...].astype(F32), gain_ref[...], shift_ref[...])
        acc_ref[...] = jnp.zeros_like(acc_ref)

    slot = load_ahead(half_loads(offsets, (u0, u1, u2, d0, d1, d2), (up_buf, down_buf), sems), first)
    up = up_buf[slot].reshape(width, up_buf.shape[-1])
    down = down_buf[slot].reshape(width, down_buf.shape[-1])
    u = jax.nn.gelu(dot_nn(h_ref[...], up) + bias_ref[0], approximate=True).astype(BF)
    acc_ref[...] += dot_nt(u, down)

    @pl.when(step == pl.num_programs(0) - 1)
    def _():
        out_ref[...] = (x_ref[...].astype(F32) + acc_ref[...] + bd_ref[...]).astype(BF)


def up_kernel(offsets, x_ref, gain_ref, shift_ref, bias_ref, u0, u1, u2, out_ref, h_ref, up_buf, sems):
    width = x_ref.shape[-1]

    def first():
        h_ref[...] = norm_rows(x_ref[...].astype(F32), gain_ref[...], shift_ref[...])

    slot = load_ahead(half_loads(offsets, (u0, u1, u2), (up_buf,), sems), first)
    up = up_buf[slot].reshape(width, up_buf.shape[-1])
    out_ref[0] = jax.nn.gelu(dot_nn(h_ref[...], up) + bias_ref[0], approximate=True).astype(BF)


def down_kernel(order, offsets, x_ref, bd_ref, u_ref, d0, d1, d2, d3, out_ref, acc_ref, down_buf, sems):
    width = x_ref.shape[-1]

    def first():
        acc_ref[...] = x_ref[...].astype(F32) + bd_ref[...]

    slot = load_ahead(half_loads(offsets, (d0, d1, d2, d3), (down_buf,), sems), first)
    acc_ref[...] += dot_nt(u_ref[0], down_buf[slot].reshape(width, down_buf.shape[-1]))

    @pl.when(pl.program_id(0) == pl.num_programs(0) - 1)
    def _():
        wl = out_ref.shape[1]
        y_t = acc_ref[...].T.astype(BF)
        for i, block in enumerate(order):
            out_ref[block] = y_t[i * wl:(i + 1) * wl]


def place_kernel(tx, ty, per, nb, *refs):
    *srcs, out_ref, sems = refs
    t, y = lax.axis_index("tx"), lax.axis_index("ty")
    copies = []
    for j, src in enumerate(srcs):
        img, dist = divmod(j, ty)
        group = y + dist - 2 * sum(bit * lax.rem(y // bit, 2) for bit in (1, 2) if dist & bit)
        for k in range(tx):
            index = group * per + lax.rem(t - k + tx, tx) * nb + img
            copies.append(pltpu.make_async_copy(src.at[k], out_ref.at[index], sems.at[j, k]))
    for copy in copies:
        copy.start()
    for copy in copies:
        copy.wait()


def solution(mesh):
    tx, ty = mesh.shape["tx"], mesh.shape["ty"]
    act_spec = P("dp", None, "tx")
    vec_tx = P(None, "tx")
    proj_spec = P(None, "tx", "ty", None)
    head_vec = P(None, "ty", None)
    in_specs = (act_spec, vec_tx, vec_tx, proj_spec, head_vec, proj_spec, proj_spec, head_vec,
                P(None, "ty", None, "tx"), vec_tx, vec_tx, vec_tx,
                P(None, "tx", "ty"), P(None, "ty"), P(None, "ty", "tx"), vec_tx)

    def local_fn(x_in, ln1_gain, ln1_bias, w_q, b_q, w_k, w_v, b_v, w_o, b_o, ln2_gain, ln2_bias, w_up, b_up, w_down, b_down):
        layers, wl, hl, dim = w_q.shape
        fl = w_up.shape[-1]
        imgs, toks, _ = x_in.shape
        hd = hl * dim
        width = wl * tx
        cols = max(4 * hd, -(-fl // LANES) * LANES)
        per = imgs // ty
        nb = per // tx
        n = nb * toks

        def proj_block(l):
            rows = [w[l].transpose(1, 2, 0).reshape(hd, wl) for w in (w_q, w_k, w_v)] + [w_o[l].reshape(hd, wl)]
            return jnp.pad(jnp.concatenate(rows, axis=0).T, ((0, 0), (0, cols - 4 * hd)))

        def up_block(l):
            return jnp.pad(w_up[l], ((0, 0), (0, cols - fl)))

        def down_block(l):
            return jnp.pad(w_down[l].T, ((0, 0), (0, cols - fl)))

        plane = lax.axis_index("dp")
        core = lax.axis_index("ty") % 2
        half = wl // 2

        order = [1, 0] + list(range(2, tx))
        groups = [[t * ty + i for t in order for i in range(ty)]]

        def blocks(a):
            return jnp.concatenate([a[i:i + 1] for i in order], axis=0)

        def gather(block):
            full = lax.all_gather(block, ("tx", "ty"), axis=0, axis_index_groups=groups)
            return full.reshape(tx, ty, *block.shape)

        halves = [("u", 0), ("d", 0), ("u", 1), ("d", 1)]
        few = wl // 72 * 16

        def half_block(block):
            return lax.dynamic_slice_in_dim(block, plane * half, half, axis=0)

        first = gather(jnp.concatenate([half_block(up_block(0)), half_block(down_block(0))], axis=0))
        last = down_block(1)
        few_rows = lax.dynamic_slice_in_dim(last, plane * few, few, axis=0)
        second = gather(jnp.concatenate([proj_block(0), half_block(up_block(1)), few_rows], axis=0))
        third = gather(proj_block(1))
        last_down = gather(last[2 * few:])
        proj = [second, third]
        split = {("u", 0): (first, 0, half), ("d", 0): (first, half, half), ("u", 1): (second, wl, half), ("d", 1): (second, wl + half, few)}

        swap = [(i, i ^ 1) for i in range(ty)]
        got, crossed = {}, {}

        def to_send(key):
            full, at, size = split[key]
            return lax.dynamic_slice(full, (core * (tx // 2), 0, at, 0), (tx // 2, ty, size, cols))

        def cross_plane(key, sent):
            got[key] = lax.ppermute(sent, "dp", [(0, 1), (1, 0)])

        def cross_core(key):
            crossed[key] = (got[key], lax.ppermute(got[key], "ty", swap))

        sent = {key: to_send(key) for key in halves[:2]}
        x_in, ln1_gain, sent = lax.optimization_barrier((x_in, ln1_gain, sent))
        cross_plane(halves[0], sent[halves[0]])
        cross_plane(halves[1], sent[halves[1]])
        images = lax.dynamic_slice_in_dim(x_in.transpose(0, 2, 1), lax.axis_index("ty") * per, per, axis=0)
        x_t = lax.all_to_all(images, "tx", split_axis=0, concat_axis=0, tiled=True)
        x = blocks(x_t.reshape(tx, nb, wl, toks)).transpose(1, 3, 0, 2).reshape(n, width)
        on_tx = [ln1_gain, ln1_bias, ln2_gain, ln2_bias, b_o, b_down]
        on_ty = [b_q.reshape(layers, hd), b_v.reshape(layers, hd), b_up]
        own = jnp.concatenate([a.reshape(1, -1) for a in on_tx + on_ty], axis=1)
        vec = lax.all_gather(own, ("tx", "ty"), axis=0)
        vec = blocks(vec.reshape(tx, ty, -1))
        at = len(on_tx) * layers * wl
        vt = vec[:, 0, :at].reshape(tx, len(on_tx), layers, wl).transpose(1, 2, 0, 3).reshape(len(on_tx), layers, 1, width)
        vq = vec[0, :, at:at + layers * hd].reshape(ty, layers, hd)
        vv = vec[0, :, at + layers * hd:at + 2 * layers * hd].reshape(ty, layers, hd)
        vu = vec[0, :, at + 2 * layers * hd:].reshape(ty, layers, fl)
        gap = jnp.zeros_like(vq)
        tail = jnp.zeros((ty, layers, cols - 4 * hd), F32)
        bias_a = jnp.concatenate([vq, gap, vv, gap, tail], axis=2).transpose(1, 0, 2).reshape(layers, ty, 1, cols)
        bias_u = jnp.pad(vu, ((0, 0), (0, 0), (0, cols - fl))).transpose(1, 0, 2).reshape(layers, ty, 1, cols)

        for key in halves[2:]:
            cross_plane(key, to_send(key))
        cross_core(halves[0])

        whole = pl.BlockSpec((n, width), lambda i: (0, 0))
        row = pl.BlockSpec((1, width), lambda i: (0, 0))
        bias = pl.BlockSpec((1, 1, cols), lambda i: (i, 0, 0))
        scratch = [pltpu.VMEM((n, width), BF), pltpu.VMEM((n, width), F32)]
        params = pltpu.CompilerParams(vmem_limit_bytes=VMEM_BYTES, dimension_semantics=("arbitrary",))

        anywhere = pl.BlockSpec(memory_space=pl.ANY)
        rows_bf, _ = scratch
        half_buf = pltpu.VMEM((2, tx, wl, cols), BF)
        act = jax.ShapeDtypeStruct((n, width), BF)
        dot_flops = 2 * n * width * cols * ty

        def kernel(fn, in_specs, out_spec, out_shape, scratch_shapes, flops):
            return pl.pallas_call(fn, grid=(ty,), in_specs=in_specs, out_specs=out_spec, out_shape=out_shape,
                                  scratch_shapes=scratch_shapes, compiler_params=params,
                                  cost_estimate=pl.CostEstimate(flops=flops, bytes_accessed=width * cols * ty * 4, transcendentals=n * cols * ty))

        for l in range(layers):
            x = kernel(lambda *refs: attention_kernel(hl, dim, toks, *refs),
                       [whole, row, row, bias, row, pl.BlockSpec((tx, 1, wl, cols), lambda i: (0, i, 0, 0))],
                       whole, act, scratch, 4 * dot_flops)(x, vt[0, l], vt[1, l], bias_a[l], vt[4, l], proj[l])
            late = halves[l + 1]
            got[late], x = lax.optimization_barrier((got[late], x))
            cross_core(late)
            up = (split["u", l][0], *crossed["u", l])
            if l < layers - 1:
                down = (split["d", l][0], *crossed["d", l])
                offsets = (split["u", l][1], split["d", l][1])
                x = kernel(lambda *refs, o=offsets: mlp_kernel(o, *refs), [whole, row, row, bias, row] + [anywhere] * 6, whole, act,
                           scratch + [half_buf, half_buf, pltpu.SemaphoreType.DMA((2, 2, 3))], 4 * dot_flops,
                           )(x, vt[2, l], vt[3, l], bias_u[l], vt[5, l], *up, *down)
            else:
                hidden = pl.BlockSpec((1, n, cols), lambda i: (i, 0, 0))
                u = kernel(lambda *refs, o=(split["u", l][1],): up_kernel(o, *refs), [whole, row, row, bias] + [anywhere] * 3, hidden,
                           jax.ShapeDtypeStruct((ty, n, cols), BF), [rows_bf, half_buf, pltpu.SemaphoreType.DMA((2, 1, 3))],
                           2 * dot_flops)(x, vt[2, l], vt[3, l], bias_u[l], *up)
                got["d", l], u = lax.optimization_barrier((got["d", l], u))
                cross_core(("d", l))
                down = (split["d", l][0], *crossed["d", l], last_down)
                outs = []
                for img in range(nb):
                    outs.append(kernel(lambda *refs, o=(split["d", l][1],): down_kernel(order, o, *refs),
                                       [pl.BlockSpec((toks, width), lambda i, m=img: (m, 0)), row,
                                        pl.BlockSpec((1, toks, cols), lambda i, m=img: (i, m, 0)),
                                        *[anywhere] * 4],
                                       pl.BlockSpec((tx, wl, toks), lambda i: (0, 0, 0)),
                                       jax.ShapeDtypeStruct((tx, wl, toks), BF),
                                       [pltpu.VMEM((toks, width), F32), half_buf, pltpu.SemaphoreType.DMA((2, 1, 4))],
                                       2 * dot_flops // nb)(x, vt[5, l], u, *down))
        me = lax.axis_index("tx")
        pieces = []
        for y_i in outs:
            moved = []
            for k in range(tx):
                part = lax.dynamic_index_in_dim(y_i, (me + k) % tx, keepdims=False)
                moved.append(lax.ppermute(part, "tx", [(i, (i + k) % tx) for i in range(tx)]) if k else part)
            by_group = [jnp.stack(moved)]
            for dist in range(1, ty):
                bit = dist & -dist
                by_group.append(lax.ppermute(by_group[dist - bit], "ty", [(i, i ^ bit) for i in range(ty)]))
            pieces += by_group
        y = pl.pallas_call(lambda *refs: place_kernel(tx, ty, per, nb, *refs),
                           in_specs=[pl.BlockSpec(memory_space=pltpu.VMEM)] * len(pieces),
                           out_specs=pl.BlockSpec(memory_space=pl.ANY),
                           out_shape=jax.ShapeDtypeStruct((imgs, wl, toks), BF),
                           scratch_shapes=[pltpu.SemaphoreType.DMA((len(pieces), tx))],
                           compiler_params=pltpu.CompilerParams(vmem_limit_bytes=VMEM_BYTES // 2), name="place")(*pieces)
        return y.transpose(0, 2, 1)

    return jax.shard_map(local_fn, mesh=mesh, in_specs=in_specs, out_specs=act_spec, check_vma=False)
```

```python
import jax
import jax.numpy as jnp
from jax import lax
from jax.experimental import pallas as pl
from jax.experimental.pallas import tpu as pltpu
from jax.sharding import PartitionSpec as P


EPS = 1e-6
BF = jnp.bfloat16
F32 = jnp.float32
LANES = 128
VMEM_BYTES = 60 * 1024 * 1024


def norm_rows(x_f, gain, shift):
    mean = jnp.mean(x_f, axis=-1, keepdims=True)
    centred = x_f - mean
    variance = jnp.mean(centred * centred, axis=-1, keepdims=True)
    return (centred * lax.rsqrt(variance + EPS) * gain + shift).astype(BF)


def dot_nn(a, b):
    return lax.dot_general(a, b, (((1,), (0,)), ((), ())), preferred_element_type=F32)


def dot_nt(a, b):
    return lax.dot_general(a, b, (((1,), (1,)), ((), ())), preferred_element_type=F32)


def attention_kernel(heads, dim, toks, x_ref, gain_ref, shift_ref, bias_ref, bo_ref, w_ref, out_ref, h_ref, acc_ref):
    step = pl.program_id(0)
    width = x_ref.shape[-1]
    hd = heads * dim
    span = -(-hd // LANES) * LANES

    @pl.when(step == 0)
    def _():
        h_ref[...] = norm_rows(x_ref[...].astype(F32), gain_ref[...], shift_ref[...])
        acc_ref[...] = jnp.zeros_like(acc_ref)

    w = w_ref[...].reshape(width, w_ref.shape[-1])
    cols = w.shape[-1]
    qkv = dot_nn(h_ref[...], w) + bias_ref[0]
    q_f = qkv[:, :span]
    k = pltpu.roll(qkv, cols - hd, 1)[:, :span].astype(BF)
    v = pltpu.roll(qkv, hd, 1)[:, cols - span:].astype(BF)
    lane = lax.broadcasted_iota(jnp.int32, (toks, span), 1)
    outs = []
    for img in range(x_ref.shape[0] // toks):
        rows = slice(img * toks, (img + 1) * toks)
        q_i, k_i, v_i = q_f[rows], k[rows], v[rows]
        o_i = jnp.zeros((toks, span), F32)
        for head in range(heads):
            q_h = jnp.where((lane >= head * dim) & (lane < (head + 1) * dim), q_i, 0.0).astype(BF)
            s = dot_nt(q_h, k_i) * (dim ** -0.5)
            e = jnp.exp(s - jnp.max(s, axis=-1, keepdims=True))
            p = (e / jnp.sum(e, axis=-1, keepdims=True)).astype(BF)
            lo = span - hd + head * dim
            o_i = jnp.where((lane >= lo) & (lane < lo + dim), dot_nn(p, v_i), o_i)
        outs.append(o_i)
    acc_ref[...] += dot_nt(jnp.concatenate(outs, axis=0).astype(BF), w[:, cols - span:])

    @pl.when(step == pl.num_programs(0) - 1)
    def _():
        out_ref[...] = (x_ref[...].astype(F32) + acc_ref[...] + bo_ref[...]).astype(BF)


def load_ahead(loads, first=lambda: None):
    step = pl.program_id(0)
    slot = lax.rem(step, 2)

    @pl.when(step == 0)
    def _():
        for copy in loads(step, slot):
            copy.start()
        first()

    @pl.when(step + 1 < pl.num_programs(0))
    def _():
        for copy in loads(step + 1, 1 - slot):
            copy.start()

    for copy in loads(step, slot):
        copy.wait()
    return slot


def half_loads(offsets, srcs, bufs, sems):
    plane = lax.axis_index("dp")
    core = lax.rem(lax.axis_index("ty"), 2)
    per = len(srcs) // len(bufs)

    def loads(i, slot):
        copies = []
        for w, buf in enumerate(bufs):
            own, same, other, *rest = srcs[per * w:per * (w + 1)]
            pair, size = same.shape[0], same.shape[2]
            mine = pl.ds(pl.multiple_of(plane * size, 16), size)
            theirs = pl.ds(pl.multiple_of((1 - plane) * size, 16), size)
            parts = [(own.at[:, i, pl.ds(offsets[w], size)], buf.at[slot, :, mine]),
                     (same.at[:, i], buf.at[slot, pl.ds(core * pair, pair), theirs]),
                     (other.at[:, i], buf.at[slot, pl.ds((1 - core) * pair, pair), theirs])]
            parts += [(r.at[:, i], buf.at[slot, :, pl.ds(2 * size, r.shape[2])]) for r in rest]
            copies += [pltpu.make_async_copy(src, dst, sems.at[slot, w, j]) for j, (src, dst) in enumerate(parts)]
        return copies

    return loads


def mlp_kernel(offsets, x_ref, gain_ref, shift_ref, bias_ref, bd_ref, u0, u1, u2, d0, d1, d2, out_ref, h_ref, acc_ref, up_buf, down_buf, sems):
    step = pl.program_id(0)
    width = x_ref.shape[-1]

    def first():
        h_ref[...] = norm_rows(x_ref[...].astype(F32), gain_ref[...], shift_ref[...])
        acc_ref[...] = jnp.zeros_like(acc_ref)

    slot = load_ahead(half_loads(offsets, (u0, u1, u2, d0, d1, d2), (up_buf, down_buf), sems), first)
    up = up_buf[slot].reshape(width, up_buf.shape[-1])
    down = down_buf[slot].reshape(width, down_buf.shape[-1])
    u = jax.nn.gelu(dot_nn(h_ref[...], up) + bias_ref[0], approximate=True).astype(BF)
    acc_ref[...] += dot_nt(u, down)

    @pl.when(step == pl.num_programs(0) - 1)
    def _():
        out_ref[...] = (x_ref[...].astype(F32) + acc_ref[...] + bd_ref[...]).astype(BF)


def up_kernel(offsets, x_ref, gain_ref, shift_ref, bias_ref, u0, u1, u2, out_ref, h_ref, up_buf, sems):
    width = x_ref.shape[-1]

    def first():
        h_ref[...] = norm_rows(x_ref[...].astype(F32), gain_ref[...], shift_ref[...])

    slot = load_ahead(half_loads(offsets, (u0, u1, u2), (up_buf,), sems), first)
    up = up_buf[slot].reshape(width, up_buf.shape[-1])
    out_ref[0] = jax.nn.gelu(dot_nn(h_ref[...], up) + bias_ref[0], approximate=True).astype(BF)


def down_kernel(order, offsets, x_ref, bd_ref, u_ref, d0, d1, d2, d3, *rest):
    *outs, acc_ref, down_buf, sems = rest
    width = x_ref.shape[-1]

    def first():
        acc_ref[...] = x_ref[...].astype(F32) + bd_ref[...]

    slot = load_ahead(half_loads(offsets, (d0, d1, d2, d3), (down_buf,), sems), first)
    acc_ref[...] += dot_nt(u_ref[0], down_buf[slot].reshape(width, down_buf.shape[-1]))

    @pl.when(pl.program_id(0) == pl.num_programs(0) - 1)
    def _():
        y_t = acc_ref[...].T.astype(BF)
        for img, out_ref in enumerate(outs):
            _, wl, toks = out_ref.shape
            for i, block in enumerate(order):
                out_ref[block] = y_t[i * wl:(i + 1) * wl, img * toks:(img + 1) * toks]


def place_kernel(tx, ty, per, nb, *refs):
    *srcs, out_ref, sems = refs
    t, y = lax.axis_index("tx"), lax.axis_index("ty")
    copies = []
    for j, src in enumerate(srcs):
        img, dist = divmod(j, ty)
        group = y + dist - 2 * sum(bit * lax.rem(y // bit, 2) for bit in (1, 2) if dist & bit)
        for k in range(tx):
            index = group * per + lax.rem(t - k + tx, tx) * nb + img
            copies.append(pltpu.make_async_copy(src.at[k], out_ref.at[index], sems.at[j, k]))
    for copy in copies:
        copy.start()
    for copy in copies:
        copy.wait()


def solution(mesh):
    tx, ty = mesh.shape["tx"], mesh.shape["ty"]
    act_spec = P("dp", None, "tx")
    vec_tx = P(None, "tx")
    proj_spec = P(None, "tx", "ty", None)
    head_vec = P(None, "ty", None)
    in_specs = (act_spec, vec_tx, vec_tx, proj_spec, head_vec, proj_spec, proj_spec, head_vec,
                P(None, "ty", None, "tx"), vec_tx, vec_tx, vec_tx,
                P(None, "tx", "ty"), P(None, "ty"), P(None, "ty", "tx"), vec_tx)

    def local_fn(x_in, ln1_gain, ln1_bias, w_q, b_q, w_k, w_v, b_v, w_o, b_o, ln2_gain, ln2_bias, w_up, b_up, w_down, b_down):
        layers, wl, hl, dim = w_q.shape
        fl = w_up.shape[-1]
        imgs, toks, _ = x_in.shape
        hd = hl * dim
        width = wl * tx
        cols = max(4 * hd, -(-fl // LANES) * LANES)
        per = imgs // ty
        nb = per // tx
        n = nb * toks

        def proj_block(l):
            rows = [w[l].transpose(1, 2, 0).reshape(hd, wl) for w in (w_q, w_k, w_v)] + [w_o[l].reshape(hd, wl)]
            return jnp.pad(jnp.concatenate(rows, axis=0).T, ((0, 0), (0, cols - 4 * hd)))

        def up_block(l):
            return jnp.pad(w_up[l], ((0, 0), (0, cols - fl)))

        def down_block(l):
            return jnp.pad(w_down[l].T, ((0, 0), (0, cols - fl)))

        plane = lax.axis_index("dp")
        core = lax.axis_index("ty") % 2
        half = wl // 2

        order = [1, 0] + list(range(2, tx))
        groups = [[t * ty + i for t in order for i in range(ty)]]

        def blocks(a):
            return jnp.concatenate([a[i:i + 1] for i in order], axis=0)

        def gather(block):
            full = lax.all_gather(block, ("tx", "ty"), axis=0, axis_index_groups=groups)
            return full.reshape(tx, ty, *block.shape)

        halves = [("u", 0), ("d", 0), ("u", 1), ("d", 1)]
        few = wl // 72 * 16

        def half_block(block):
            return lax.dynamic_slice_in_dim(block, plane * half, half, axis=0)

        first = gather(jnp.concatenate([half_block(up_block(0)), half_block(down_block(0))], axis=0))
        last = down_block(1)
        few_rows = lax.dynamic_slice_in_dim(last, plane * few, few, axis=0)
        second = gather(jnp.concatenate([proj_block(0), half_block(up_block(1)), few_rows], axis=0))
        third = gather(proj_block(1))
        last_down = gather(last[2 * few:])
        proj = [second, third]
        split = {("u", 0): (first, 0, half), ("d", 0): (first, half, half), ("u", 1): (second, wl, half), ("d", 1): (second, wl + half, few)}

        swap = [(i, i ^ 1) for i in range(ty)]
        got, crossed = {}, {}

        def to_send(key):
            full, at, size = split[key]
            return lax.dynamic_slice(full, (core * (tx // 2), 0, at, 0), (tx // 2, ty, size, cols))

        def cross_plane(key, sent):
            got[key] = lax.ppermute(sent, "dp", [(0, 1), (1, 0)])

        def cross_core(key):
            crossed[key] = (got[key], lax.ppermute(got[key], "ty", swap))

        sent = {key: to_send(key) for key in halves[:2]}
        x_in, ln1_gain, sent = lax.optimization_barrier((x_in, ln1_gain, sent))
        cross_plane(halves[0], sent[halves[0]])
        cross_plane(halves[1], sent[halves[1]])
        images = lax.dynamic_slice_in_dim(x_in.transpose(0, 2, 1), lax.axis_index("ty") * per, per, axis=0)
        x_t = lax.all_to_all(images, "tx", split_axis=0, concat_axis=0, tiled=True)
        x = blocks(x_t.reshape(tx, nb, wl, toks)).transpose(1, 3, 0, 2).reshape(n, width)
        on_tx = [ln1_gain, ln1_bias, ln2_gain, ln2_bias, b_o, b_down]
        on_ty = [b_q.reshape(layers, hd), b_v.reshape(layers, hd), b_up]
        own = jnp.concatenate([a.reshape(1, -1) for a in on_tx + on_ty], axis=1)
        vec = lax.all_gather(own, ("tx", "ty"), axis=0)
        vec = blocks(vec.reshape(tx, ty, -1))
        at = len(on_tx) * layers * wl
        vt = vec[:, 0, :at].reshape(tx, len(on_tx), layers, wl).transpose(1, 2, 0, 3).reshape(len(on_tx), layers, 1, width)
        vq = vec[0, :, at:at + layers * hd].reshape(ty, layers, hd)
        vv = vec[0, :, at + layers * hd:at + 2 * layers * hd].reshape(ty, layers, hd)
        vu = vec[0, :, at + 2 * layers * hd:].reshape(ty, layers, fl)
        gap = jnp.zeros_like(vq)
        tail = jnp.zeros((ty, layers, cols - 4 * hd), F32)
        bias_a = jnp.concatenate([vq, gap, vv, gap, tail], axis=2).transpose(1, 0, 2).reshape(layers, ty, 1, cols)
        bias_u = jnp.pad(vu, ((0, 0), (0, 0), (0, cols - fl))).transpose(1, 0, 2).reshape(layers, ty, 1, cols)

        for key in halves[2:]:
            cross_plane(key, to_send(key))
        cross_core(halves[0])

        whole = pl.BlockSpec((n, width), lambda i: (0, 0))
        row = pl.BlockSpec((1, width), lambda i: (0, 0))
        bias = pl.BlockSpec((1, 1, cols), lambda i: (i, 0, 0))
        scratch = [pltpu.VMEM((n, width), BF), pltpu.VMEM((n, width), F32)]
        params = pltpu.CompilerParams(vmem_limit_bytes=VMEM_BYTES, dimension_semantics=("arbitrary",))

        anywhere = pl.BlockSpec(memory_space=pl.ANY)
        rows_bf, rows_f = scratch
        half_buf = pltpu.VMEM((2, tx, wl, cols), BF)
        act = jax.ShapeDtypeStruct((n, width), BF)
        dot_flops = 2 * n * width * cols * ty

        def kernel(fn, in_specs, out_spec, out_shape, scratch_shapes, flops):
            return pl.pallas_call(fn, grid=(ty,), in_specs=in_specs, out_specs=out_spec, out_shape=out_shape,
                                  scratch_shapes=scratch_shapes, compiler_params=params,
                                  cost_estimate=pl.CostEstimate(flops=flops, bytes_accessed=width * cols * ty * 4, transcendentals=n * cols * ty))

        for l in range(layers):
            if l:
                got["u", l], x = lax.optimization_barrier((got["u", l], x))
                cross_core(("u", l))
            x = kernel(lambda *refs: attention_kernel(hl, dim, toks, *refs),
                       [whole, row, row, bias, row, pl.BlockSpec((tx, 1, wl, cols), lambda i: (0, i, 0, 0))],
                       whole, act, scratch, 4 * dot_flops)(x, vt[0, l], vt[1, l], bias_a[l], vt[4, l], proj[l])
            late = halves[2 * l + 1]
            got[late], x = lax.optimization_barrier((got[late], x))
            cross_core(late)
            up = (split["u", l][0], *crossed["u", l])
            if l < layers - 1:
                down = (split["d", l][0], *crossed["d", l])
                offsets = (split["u", l][1], split["d", l][1])
                x = kernel(lambda *refs, o=offsets: mlp_kernel(o, *refs), [whole, row, row, bias, row] + [anywhere] * 6, whole, act,
                           scratch + [half_buf, half_buf, pltpu.SemaphoreType.DMA((2, 2, 3))], 4 * dot_flops,
                           )(x, vt[2, l], vt[3, l], bias_u[l], vt[5, l], *up, *down)
            else:
                hidden = pl.BlockSpec((1, n, cols), lambda i: (i, 0, 0))
                u = kernel(lambda *refs, o=(split["u", l][1],): up_kernel(o, *refs), [whole, row, row, bias] + [anywhere] * 3, hidden,
                           jax.ShapeDtypeStruct((ty, n, cols), BF), [rows_bf, half_buf, pltpu.SemaphoreType.DMA((2, 1, 3))],
                           2 * dot_flops)(x, vt[2, l], vt[3, l], bias_u[l], *up)
                down = (split["d", l][0], *crossed["d", l], last_down)
                outs = kernel(lambda *refs, o=(split["d", l][1],): down_kernel(order, o, *refs),
                              [whole, row, hidden] + [anywhere] * 4,
                              [pl.BlockSpec((tx, wl, toks), lambda i: (0, 0, 0))] * nb,
                              [jax.ShapeDtypeStruct((tx, wl, toks), BF)] * nb,
                              [rows_f, half_buf, pltpu.SemaphoreType.DMA((2, 1, 4))], 2 * dot_flops)(x, vt[5, l], u, *down)
        me = lax.axis_index("tx")
        pieces = []
        for y_i in outs:
            moved = []
            for k in range(tx):
                part = lax.dynamic_index_in_dim(y_i, (me + k) % tx, keepdims=False)
                moved.append(lax.ppermute(part, "tx", [(i, (i + k) % tx) for i in range(tx)]) if k else part)
            by_group = [jnp.stack(moved)]
            for dist in range(1, ty):
                bit = dist & -dist
                by_group.append(lax.ppermute(by_group[dist - bit], "ty", [(i, i ^ bit) for i in range(ty)]))
            pieces += by_group
        y = pl.pallas_call(lambda *refs: place_kernel(tx, ty, per, nb, *refs),
                           in_specs=[pl.BlockSpec(memory_space=pltpu.VMEM)] * len(pieces),
                           out_specs=pl.BlockSpec(memory_space=pl.ANY),
                           out_shape=jax.ShapeDtypeStruct((imgs, wl, toks), BF),
                           scratch_shapes=[pltpu.SemaphoreType.DMA((len(pieces), tx))],
                           compiler_params=pltpu.CompilerParams(vmem_limit_bytes=VMEM_BYTES // 2), name="place")(*pieces)
        return y.transpose(0, 2, 1)

    return jax.shard_map(local_fn, mesh=mesh, in_specs=in_specs, out_specs=act_spec, check_vma=False)
```

```python
import jax
import jax.numpy as jnp
from jax import lax
from jax.experimental import pallas as pl
from jax.experimental.pallas import tpu as pltpu
from jax.sharding import PartitionSpec as P


EPS = 1e-6
BF = jnp.bfloat16
F32 = jnp.float32
LANES = 128
VMEM_BYTES = 60 * 1024 * 1024


def norm_rows(x_f, gain, shift):
    mean = jnp.mean(x_f, axis=-1, keepdims=True)
    centred = x_f - mean
    variance = jnp.mean(centred * centred, axis=-1, keepdims=True)
    return (centred * lax.rsqrt(variance + EPS) * gain + shift).astype(BF)


def dot_nn(a, b):
    return lax.dot_general(a, b, (((1,), (0,)), ((), ())), preferred_element_type=F32)


def dot_nt(a, b):
    return lax.dot_general(a, b, (((1,), (1,)), ((), ())), preferred_element_type=F32)


def attention_kernel(heads, dim, toks, x_ref, gain_ref, shift_ref, bias_ref, bo_ref, w_ref, out_ref, h_ref, acc_ref):
    step = pl.program_id(0)
    width = x_ref.shape[-1]
    hd = heads * dim
    span = -(-hd // LANES) * LANES

    @pl.when(step == 0)
    def _():
        h_ref[...] = norm_rows(x_ref[...].astype(F32), gain_ref[...], shift_ref[...])
        acc_ref[...] = jnp.zeros_like(acc_ref)

    w = w_ref[...].reshape(width, w_ref.shape[-1])
    cols = w.shape[-1]
    qkv = dot_nn(h_ref[...], w) + bias_ref[0]
    q_f = qkv[:, :span]
    k = pltpu.roll(qkv, cols - hd, 1)[:, :span].astype(BF)
    v = pltpu.roll(qkv, hd, 1)[:, cols - span:].astype(BF)
    lane = lax.broadcasted_iota(jnp.int32, (toks, span), 1)
    outs = []
    for img in range(x_ref.shape[0] // toks):
        rows = slice(img * toks, (img + 1) * toks)
        q_i, k_i, v_i = q_f[rows], k[rows], v[rows]
        o_i = jnp.zeros((toks, span), F32)
        for head in range(heads):
            q_h = jnp.where((lane >= head * dim) & (lane < (head + 1) * dim), q_i, 0.0).astype(BF)
            s = dot_nt(q_h, k_i) * (dim ** -0.5)
            e = jnp.exp(s - jnp.max(s, axis=-1, keepdims=True))
            p = (e / jnp.sum(e, axis=-1, keepdims=True)).astype(BF)
            lo = span - hd + head * dim
            o_i = jnp.where((lane >= lo) & (lane < lo + dim), dot_nn(p, v_i), o_i)
        outs.append(o_i)
    acc_ref[...] += dot_nt(jnp.concatenate(outs, axis=0).astype(BF), w[:, cols - span:])

    @pl.when(step == pl.num_programs(0) - 1)
    def _():
        out_ref[...] = (x_ref[...].astype(F32) + acc_ref[...] + bo_ref[...]).astype(BF)


def load_ahead(loads, first=lambda: None):
    step = pl.program_id(0)
    slot = lax.rem(step, 2)

    @pl.when(step == 0)
    def _():
        for copy in loads(step, slot):
            copy.start()
        first()

    @pl.when(step + 1 < pl.num_programs(0))
    def _():
        for copy in loads(step + 1, 1 - slot):
            copy.start()

    for copy in loads(step, slot):
        copy.wait()
    return slot


def half_loads(offsets, srcs, bufs, sems):
    plane = lax.axis_index("dp")
    core = lax.rem(lax.axis_index("ty"), 2)
    per = len(srcs) // len(bufs)

    def loads(i, slot):
        copies = []
        for w, buf in enumerate(bufs):
            own, same, other, *rest = srcs[per * w:per * (w + 1)]
            pair, size = same.shape[0], same.shape[2]
            mine = pl.ds(pl.multiple_of(plane * size, 16), size)
            theirs = pl.ds(pl.multiple_of((1 - plane) * size, 16), size)
            parts = [(own.at[:, i, pl.ds(offsets[w], size)], buf.at[slot, :, mine]),
                     (same.at[:, i], buf.at[slot, pl.ds(core * pair, pair), theirs]),
                     (other.at[:, i], buf.at[slot, pl.ds((1 - core) * pair, pair), theirs])]
            parts += [(r.at[:, i], buf.at[slot, :, pl.ds(2 * size, r.shape[2])]) for r in rest]
            copies += [pltpu.make_async_copy(src, dst, sems.at[slot, w, j]) for j, (src, dst) in enumerate(parts)]
        return copies

    return loads


def mlp_kernel(offsets, x_ref, gain_ref, shift_ref, bias_ref, bd_ref, u0, u1, u2, d0, d1, d2, out_ref, h_ref, acc_ref, up_buf, down_buf, sems):
    step = pl.program_id(0)
    width = x_ref.shape[-1]

    def first():
        h_ref[...] = norm_rows(x_ref[...].astype(F32), gain_ref[...], shift_ref[...])
        acc_ref[...] = jnp.zeros_like(acc_ref)

    slot = load_ahead(half_loads(offsets, (u0, u1, u2, d0, d1, d2), (up_buf, down_buf), sems), first)
    up = up_buf[slot].reshape(width, up_buf.shape[-1])
    down = down_buf[slot].reshape(width, down_buf.shape[-1])
    u = jax.nn.gelu(dot_nn(h_ref[...], up) + bias_ref[0], approximate=True).astype(BF)
    acc_ref[...] += dot_nt(u, down)

    @pl.when(step == pl.num_programs(0) - 1)
    def _():
        out_ref[...] = (x_ref[...].astype(F32) + acc_ref[...] + bd_ref[...]).astype(BF)


def up_kernel(offsets, x_ref, gain_ref, shift_ref, bias_ref, u0, u1, u2, out_ref, h_ref, up_buf, sems):
    width = x_ref.shape[-1]

    def first():
        h_ref[...] = norm_rows(x_ref[...].astype(F32), gain_ref[...], shift_ref[...])

    slot = load_ahead(half_loads(offsets, (u0, u1, u2), (up_buf,), sems), first)
    up = up_buf[slot].reshape(width, up_buf.shape[-1])
    out_ref[0] = jax.nn.gelu(dot_nn(h_ref[...], up) + bias_ref[0], approximate=True).astype(BF)


def down_kernel(order, offsets, x_ref, bd_ref, u_ref, d0, d1, d2, d3, out_ref, acc_ref, down_buf, sems):
    width = x_ref.shape[-1]

    def first():
        acc_ref[...] = x_ref[...].astype(F32) + bd_ref[...]

    slot = load_ahead(half_loads(offsets, (d0, d1, d2, d3), (down_buf,), sems), first)
    acc_ref[...] += dot_nt(u_ref[0], down_buf[slot].reshape(width, down_buf.shape[-1]))

    @pl.when(pl.program_id(0) == pl.num_programs(0) - 1)
    def _():
        wl = out_ref.shape[1]
        y_t = acc_ref[...].T.astype(BF)
        for i, block in enumerate(order):
            out_ref[block] = y_t[i * wl:(i + 1) * wl]


def place_kernel(tx, ty, per, nb, *refs):
    *srcs, out_ref, sems = refs
    t, y = lax.axis_index("tx"), lax.axis_index("ty")
    copies = []
    for j, src in enumerate(srcs):
        img, dist = divmod(j, ty)
        group = y + dist - 2 * sum(bit * lax.rem(y // bit, 2) for bit in (1, 2) if dist & bit)
        for k in range(tx):
            index = group * per + lax.rem(t - k + tx, tx) * nb + img
            copies.append(pltpu.make_async_copy(src.at[k], out_ref.at[index], sems.at[j, k]))
    for copy in copies:
        copy.start()
    for copy in copies:
        copy.wait()


def solution(mesh):
    tx, ty = mesh.shape["tx"], mesh.shape["ty"]
    act_spec = P("dp", None, "tx")
    vec_tx = P(None, "tx")
    proj_spec = P(None, "tx", "ty", None)
    head_vec = P(None, "ty", None)
    in_specs = (act_spec, vec_tx, vec_tx, proj_spec, head_vec, proj_spec, proj_spec, head_vec,
                P(None, "ty", None, "tx"), vec_tx, vec_tx, vec_tx,
                P(None, "tx", "ty"), P(None, "ty"), P(None, "ty", "tx"), vec_tx)

    def local_fn(x_in, ln1_gain, ln1_bias, w_q, b_q, w_k, w_v, b_v, w_o, b_o, ln2_gain, ln2_bias, w_up, b_up, w_down, b_down):
        layers, wl, hl, dim = w_q.shape
        fl = w_up.shape[-1]
        imgs, toks, _ = x_in.shape
        hd = hl * dim
        width = wl * tx
        cols = max(4 * hd, -(-fl // LANES) * LANES)
        per = imgs // ty
        nb = per // tx
        n = nb * toks

        def proj_block(l):
            rows = [w[l].transpose(1, 2, 0).reshape(hd, wl) for w in (w_q, w_k, w_v)] + [w_o[l].reshape(hd, wl)]
            return jnp.pad(jnp.concatenate(rows, axis=0).T, ((0, 0), (0, cols - 4 * hd)))

        def up_block(l):
            return jnp.pad(w_up[l], ((0, 0), (0, cols - fl)))

        def down_block(l):
            return jnp.pad(w_down[l].T, ((0, 0), (0, cols - fl)))

        plane = lax.axis_index("dp")
        core = lax.axis_index("ty") % 2
        half = wl // 2

        order = [1, 0] + list(range(2, tx))
        groups = [[t * ty + i for t in order for i in range(ty)]]

        def blocks(a):
            return jnp.concatenate([a[i:i + 1] for i in order], axis=0)

        def gather(block):
            full = lax.all_gather(block, ("tx", "ty"), axis=0, axis_index_groups=groups)
            return full.reshape(tx, ty, *block.shape)

        halves = [("u", 0), ("d", 0), ("u", 1), ("d", 1)]
        few = wl // 72 * 16

        def half_block(block):
            return lax.dynamic_slice_in_dim(block, plane * half, half, axis=0)

        first = gather(jnp.concatenate([half_block(up_block(0)), half_block(down_block(0))], axis=0))
        last = down_block(1)
        few_rows = lax.dynamic_slice_in_dim(last, plane * few, few, axis=0)
        second = gather(jnp.concatenate([proj_block(0), half_block(up_block(1)), few_rows], axis=0))
        third = gather(proj_block(1))
        last_down = gather(last[2 * few:])
        proj = [second, third]
        split = {("u", 0): (first, 0, half), ("d", 0): (first, half, half), ("u", 1): (second, wl, half), ("d", 1): (second, wl + half, few)}

        swap = [(i, i ^ 1) for i in range(ty)]
        got, crossed = {}, {}

        def to_send(key):
            full, at, size = split[key]
            return lax.dynamic_slice(full, (core * (tx // 2), 0, at, 0), (tx // 2, ty, size, cols))

        def cross_plane(key, sent):
            got[key] = lax.ppermute(sent, "dp", [(0, 1), (1, 0)])

        def cross_core(key):
            crossed[key] = (got[key], lax.ppermute(got[key], "ty", swap))

        sent = {key: to_send(key) for key in halves[:2]}
        x_in, ln1_gain, sent = lax.optimization_barrier((x_in, ln1_gain, sent))
        cross_plane(halves[0], sent[halves[0]])
        cross_plane(halves[1], sent[halves[1]])
        images = lax.dynamic_slice_in_dim(x_in.transpose(0, 2, 1), lax.axis_index("ty") * per, per, axis=0)
        x_t = lax.all_to_all(images, "tx", split_axis=0, concat_axis=0, tiled=True)
        x = blocks(x_t.reshape(tx, nb, wl, toks)).transpose(1, 3, 0, 2).reshape(n, width)
        on_tx = [ln1_gain, ln1_bias, ln2_gain, ln2_bias, b_o, b_down]
        on_ty = [b_q.reshape(layers, hd), b_v.reshape(layers, hd), b_up]
        own = jnp.concatenate([a.reshape(1, -1) for a in on_tx + on_ty], axis=1)
        vec = lax.all_gather(own, ("tx", "ty"), axis=0)
        vec = blocks(vec.reshape(tx, ty, -1))
        at = len(on_tx) * layers * wl
        vt = vec[:, 0, :at].reshape(tx, len(on_tx), layers, wl).transpose(1, 2, 0, 3).reshape(len(on_tx), layers, 1, width)
        vq = vec[0, :, at:at + layers * hd].reshape(ty, layers, hd)
        vv = vec[0, :, at + layers * hd:at + 2 * layers * hd].reshape(ty, layers, hd)
        vu = vec[0, :, at + 2 * layers * hd:].reshape(ty, layers, fl)
        gap = jnp.zeros_like(vq)
        tail = jnp.zeros((ty, layers, cols - 4 * hd), F32)
        bias_a = jnp.concatenate([vq, gap, vv, gap, tail], axis=2).transpose(1, 0, 2).reshape(layers, ty, 1, cols)
        bias_u = jnp.pad(vu, ((0, 0), (0, 0), (0, cols - fl))).transpose(1, 0, 2).reshape(layers, ty, 1, cols)

        for key in halves[2:]:
            cross_plane(key, to_send(key))
        cross_core(halves[0])

        whole = pl.BlockSpec((n, width), lambda i: (0, 0))
        row = pl.BlockSpec((1, width), lambda i: (0, 0))
        bias = pl.BlockSpec((1, 1, cols), lambda i: (i, 0, 0))
        scratch = [pltpu.VMEM((n, width), BF), pltpu.VMEM((n, width), F32)]
        params = pltpu.CompilerParams(vmem_limit_bytes=VMEM_BYTES, dimension_semantics=("arbitrary",))

        anywhere = pl.BlockSpec(memory_space=pl.ANY)
        rows_bf, _ = scratch
        half_buf = pltpu.VMEM((2, tx, wl, cols), BF)
        act = jax.ShapeDtypeStruct((n, width), BF)
        dot_flops = 2 * n * width * cols * ty

        def kernel(fn, in_specs, out_spec, out_shape, scratch_shapes, flops):
            return pl.pallas_call(fn, grid=(ty,), in_specs=in_specs, out_specs=out_spec, out_shape=out_shape,
                                  scratch_shapes=scratch_shapes, compiler_params=params,
                                  cost_estimate=pl.CostEstimate(flops=flops, bytes_accessed=width * cols * ty * 4, transcendentals=n * cols * ty))

        for l in range(layers):
            if l:
                got["u", l], x = lax.optimization_barrier((got["u", l], x))
                cross_core(("u", l))
            x = kernel(lambda *refs: attention_kernel(hl, dim, toks, *refs),
                       [whole, row, row, bias, row, pl.BlockSpec((tx, 1, wl, cols), lambda i: (0, i, 0, 0))],
                       whole, act, scratch, 4 * dot_flops)(x, vt[0, l], vt[1, l], bias_a[l], vt[4, l], proj[l])
            late = halves[2 * l + 1]
            got[late], x = lax.optimization_barrier((got[late], x))
            cross_core(late)
            up = (split["u", l][0], *crossed["u", l])
            if l < layers - 1:
                down = (split["d", l][0], *crossed["d", l])
                offsets = (split["u", l][1], split["d", l][1])
                x = kernel(lambda *refs, o=offsets: mlp_kernel(o, *refs), [whole, row, row, bias, row] + [anywhere] * 6, whole, act,
                           scratch + [half_buf, half_buf, pltpu.SemaphoreType.DMA((2, 2, 3))], 4 * dot_flops,
                           )(x, vt[2, l], vt[3, l], bias_u[l], vt[5, l], *up, *down)
            else:
                hidden = pl.BlockSpec((1, n, cols), lambda i: (i, 0, 0))
                u = kernel(lambda *refs, o=(split["u", l][1],): up_kernel(o, *refs), [whole, row, row, bias] + [anywhere] * 3, hidden,
                           jax.ShapeDtypeStruct((ty, n, cols), BF), [rows_bf, half_buf, pltpu.SemaphoreType.DMA((2, 1, 3))],
                           2 * dot_flops)(x, vt[2, l], vt[3, l], bias_u[l], *up)
                down = (split["d", l][0], *crossed["d", l], last_down)
                outs = []
                for img in range(nb):
                    outs.append(kernel(lambda *refs, o=(split["d", l][1],): down_kernel(order, o, *refs),
                                       [pl.BlockSpec((toks, width), lambda i, m=img: (m, 0)), row,
                                        pl.BlockSpec((1, toks, cols), lambda i, m=img: (i, m, 0)),
                                        *[anywhere] * 4],
                                       pl.BlockSpec((tx, wl, toks), lambda i: (0, 0, 0)),
                                       jax.ShapeDtypeStruct((tx, wl, toks), BF),
                                       [pltpu.VMEM((toks, width), F32), half_buf, pltpu.SemaphoreType.DMA((2, 1, 4))],
                                       2 * dot_flops // nb)(x, vt[5, l], u, *down))
        me = lax.axis_index("tx")
        pieces = []
        for y_i in outs:
            moved = []
            for k in range(tx):
                part = lax.dynamic_index_in_dim(y_i, (me + k) % tx, keepdims=False)
                moved.append(lax.ppermute(part, "tx", [(i, (i + k) % tx) for i in range(tx)]) if k else part)
            by_group = [jnp.stack(moved)]
            for dist in range(1, ty):
                bit = dist & -dist
                by_group.append(lax.ppermute(by_group[dist - bit], "ty", [(i, i ^ bit) for i in range(ty)]))
            pieces += by_group
        y = pl.pallas_call(lambda *refs: place_kernel(tx, ty, per, nb, *refs),
                           in_specs=[pl.BlockSpec(memory_space=pltpu.VMEM)] * len(pieces),
                           out_specs=pl.BlockSpec(memory_space=pl.ANY),
                           out_shape=jax.ShapeDtypeStruct((imgs, wl, toks), BF),
                           scratch_shapes=[pltpu.SemaphoreType.DMA((len(pieces), tx))],
                           compiler_params=pltpu.CompilerParams(vmem_limit_bytes=VMEM_BYTES // 2), name="place")(*pieces)
        return y.transpose(0, 2, 1)

    return jax.shard_map(local_fn, mesh=mesh, in_specs=in_specs, out_specs=act_spec, check_vma=False)
```
